128 devices in a mesh: px: 8 (over x, z_lo), py: 16 (over z_hi, y, core).
Axes of the slice: x: 4, y: 4, z: 4 (z_hi: 2, z_lo: 2; z = z_hi * 2 + z_lo), core: 2. Of those that a mesh axis runs over, the one named last changes fastest.
Arguments:
- velocity: float32 [3, 8, 512, 2048], P(None, None, 'py', 'px'), may hold values from -6 to 6
- thickness: float32 [8, 512, 2048], P(None, 'py', 'px'), may hold values from 1 to 4
- velocity_tendency: float32 [3, 8, 512, 2048], P(None, None, 'py', 'px'), may hold values from -6 to 6
- thickness_tendency: float32 [8, 512, 2048], P(None, 'py', 'px'), may hold values from -0.5 to 0.5
- cell_distance: float32 [3, 512, 2048], P(None, 'py', 'px'), may hold values from 0.5 to 2
- edge_length: float32 [3, 512, 2048], P(None, 'py', 'px'), may hold values from 0.5 to 2
- cell_area: float32 [512, 2048], P('py', 'px'), may hold values from 1 to 4
- kite_area: float32 [2, 3, 512, 2048], P(None, None, 'py', 'px'), may hold values from 0.2 to 0.8
- coriolis: float32 [2, 512, 2048], P(None, 'py', 'px'), may hold values from -1 to 1
Outputs:
- vertex_potential: float32 [2, 8, 512, 2048], P(None, None, 'py', 'px')
- kinetic_energy: float32 [8, 512, 2048], P(None, 'py', 'px')
- cell_potential: float32 [8, 512, 2048], P(None, 'py', 'px')
- edge_potential: float32 [3, 8, 512, 2048], P(None, None, 'py', 'px')
The draws below stay inside these ranges and needn't reach their ends.
All inputs are finite; a program needn't handle non-finite values.
Results may differ from the reference program's by a relative error of at most 0.00002.
Values sent between devices are 32-bit elements; how exact they have to be, the bound alone decides.
A program may use at most 64 MiB of HBM per device.

```python
import math
import jax
import jax.numpy as jnp

NLEV = 8
SECTIONS = 4
NX = 512
NY = 2048


def levels(key, shape, split, least, top_value):
    def one(position, blocks):
        draws = jax.random.uniform(jax.random.fold_in(jax.random.fold_in(key, 6), position), (blocks,), jnp.float32, least / len(split), top_value / len(split))
        return jnp.repeat(jnp.exp(draws), shape[position] // blocks).reshape((-1,) + (1,) * (len(shape) - position - 1))

    loudness = one(*split[0])
    for cut in split[1:]:
        loudness = loudness * one(*cut)
    return loudness


def noise(own_key, extent, scale, bound, shards=(), dtype=jnp.bfloat16):
    values = scale * jax.random.normal(own_key, extent, jnp.float32)
    if shards:
        values = values * levels(own_key, extent, shards, -0.22, 0.18)
    return jnp.clip(values, -bound, bound).astype(dtype)


def setup_inputs(seed: int = 0) -> dict:
    arg_keys = jax.random.split(jax.random.key(seed), 10)
    velocity = noise(arg_keys[0], (3, NLEV, NX, NY), 1.0, 6.0, ((2, 16), (3, 8)), jnp.float32)
    thickness = jnp.clip(jnp.exp(math.log(4.0) - 1.3862944 * jax.random.uniform(arg_keys[1], (NLEV, NX, NY), jnp.float32) ** levels(arg_keys[1], (NLEV, NX, NY), ((1, 16), (2, 8)), -0.2, 0.2)), 1.0, 4.0)
    velocity_tendency = noise(arg_keys[2], (3, NLEV, NX, NY), 1.0, 6.0, ((2, 16), (3, 8)), jnp.float32)
    thickness_tendency = jnp.clip(jax.random.uniform(arg_keys[3], (NLEV, NX, NY), jnp.float32, -0.5, 0.5) * levels(arg_keys[3], (NLEV, NX, NY), ((1, 16), (2, 8)), -0.4, 0.0), -0.5, 0.5)
    cell_distance = jnp.clip(jnp.exp(math.log(2.0) - 1.3862944 * jax.random.uniform(arg_keys[4], (3, NX, NY), jnp.float32) ** levels(arg_keys[4], (3, NX, NY), ((1, 16), (2, 8)), -0.2, 0.2)), 0.5, 2.0)
    edge_length = jnp.clip(jnp.exp(math.log(2.0) - 1.3862944 * jax.random.uniform(arg_keys[5], (3, NX, NY), jnp.float32) ** levels(arg_keys[5], (3, NX, NY), ((1, 16), (2, 8)), -0.2, 0.2)), 0.5, 2.0)
    cell_area = jnp.clip(jnp.exp(math.log(4.0) - 1.3862944 * jax.random.uniform(arg_keys[6], (NX, NY), jnp.float32) ** levels(arg_keys[6], (NX, NY), ((0, 16), (1, 8)), -0.2, 0.2)), 1.0, 4.0)
    kite_area = jnp.clip(jnp.exp(math.log(0.8) - 1.3862944 * jax.random.uniform(arg_keys[7], (2, 3, NX, NY), jnp.float32) ** levels(arg_keys[7], (2, 3, NX, NY), ((2, 16), (3, 8)), -0.2, 0.2)), 0.2, 0.8)
    coriolis = jnp.clip(jax.random.uniform(arg_keys[8], (2, NX, NY), jnp.float32, -1.0, 1.0) * levels(arg_keys[8], (2, NX, NY), ((1, 16), (2, 8)), -0.4, 0.0), -1.0, 1.0)
    return dict(velocity=velocity, thickness=thickness, velocity_tendency=velocity_tendency, thickness_tendency=thickness_tendency, cell_distance=cell_distance, edge_length=edge_length, cell_area=cell_area, kite_area=kite_area, coriolis=coriolis)


SECTION_STEP = (0.0, 0.5, 0.5, 1.0)
SECTION_WEIGHT = (1.0 / 6.0, 1.0 / 3.0, 1.0 / 3.0, 1.0 / 6.0)
UPWIND_FACTOR = 0.5


def neighbour(field, first_off, second_off):
    return jnp.roll(field, (-first_off, -second_off), axis=(-2, -1))


def reference(velocity, thickness, velocity_tendency, thickness_tendency, cell_distance, edge_length, cell_area, kite_area, coriolis):
    triangle_area = jnp.sum(kite_area, axis=1)
    edge_weight = 0.25 * cell_distance * edge_length
    vertex_total = jnp.zeros((2,) + thickness.shape, jnp.float32)
    energy_total = jnp.zeros(thickness.shape, jnp.float32)
    cell_total = jnp.zeros(thickness.shape, jnp.float32)
    edge_total = jnp.zeros(velocity.shape, jnp.float32)
    for section_index in range(SECTIONS):
        step_size = SECTION_STEP[section_index]
        weight_now = SECTION_WEIGHT[section_index]
        section_velocity = velocity + step_size * velocity_tendency
        section_thickness = thickness + step_size * thickness_tendency
        edge_flux = section_velocity * cell_distance[:, None]
        circulation_first = edge_flux[0] + neighbour(edge_flux[2], 1, 0) - edge_flux[1]
        circulation_second = edge_flux[1] - edge_flux[2] - neighbour(edge_flux[0], -1, 1)
        height_first = (kite_area[0, 0] * section_thickness + kite_area[0, 1] * neighbour(section_thickness, 1, 0)
                        + kite_area[0, 2] * neighbour(section_thickness, 0, 1)) / triangle_area[0]
        height_second = (kite_area[1, 0] * section_thickness + kite_area[1, 1] * neighbour(section_thickness, 0, 1)
                         + kite_area[1, 2] * neighbour(section_thickness, -1, 1)) / triangle_area[1]
        potential_first = (coriolis[0] + circulation_first / triangle_area[0]) / height_first
        potential_second = (coriolis[1] + circulation_second / triangle_area[1]) / height_second
        energy = edge_weight[:, None] * section_velocity * section_velocity
        kinetic = (energy[0] + energy[1] + energy[2] + neighbour(energy[0], -1, 0)
                   + neighbour(energy[1], 0, -1) + neighbour(energy[2], 1, -1)) / cell_area
        cell_value = (potential_first + potential_second + neighbour(potential_first, -1, 0)
                      + neighbour(potential_first, 0, -1) + neighbour(potential_second, 0, -1)
                      + neighbour(potential_second, 1, -1)) / 6.0
        mean_zero = 0.5 * (potential_first + neighbour(potential_second, 1, -1))
        mean_one = 0.5 * (potential_first + potential_second)
        mean_two = 0.5 * (potential_second + neighbour(potential_first, -1, 0))
        grad_zero = (neighbour(cell_value, 1, 0) - cell_value) / cell_distance[0]
        grad_one = (neighbour(cell_value, 0, 1) - cell_value) / cell_distance[1]
        grad_two = (neighbour(cell_value, -1, 1) - cell_value) / cell_distance[2]
        section_edge = jnp.stack([
            mean_zero - UPWIND_FACTOR * section_velocity[0] * grad_zero,
            mean_one - UPWIND_FACTOR * section_velocity[1] * grad_one,
            mean_two - UPWIND_FACTOR * section_velocity[2] * grad_two])
        vertex_total = vertex_total + weight_now * jnp.stack([potential_first, potential_second])
        energy_total = energy_total + weight_now * kinetic
        cell_total = cell_total + weight_now * cell_value
        edge_total = edge_total + weight_now * section_edge
    return vertex_total, energy_total, cell_total, edge_total
```

```python
import jax
import jax.numpy as jnp
from jax import lax
from jax.experimental import pallas as pl
from jax.experimental.pallas import tpu as pltpu
from jax.sharding import PartitionSpec as P

F32 = jnp.float32
MESH = pl.DeviceIdType.MESH
ROWS = 32
EXT = ROWS + 4
LEVELS = 8
LANES = 128

FIRST = (-2, 12, 26)
FIELDS = 10

DOWN, UP, RIGHT, LEFT = (1, 0), (-1, 0), (0, 1), (0, -1)
DOWN_LEFT, UP_LEFT, UP_RIGHT = (1, -1), (-1, -1), (-1, 1)
TARGETS = (DOWN, UP, RIGHT, LEFT, DOWN_LEFT, UP_LEFT, UP_RIGHT)


def rim_of(row):
    block = 0 if row <= 12 else (1 if row <= 26 else 2)
    return block, (row - FIRST[block]) * 8


def lane_id():
    return lax.broadcasted_iota(jnp.int32, (LEVELS, LANES), 1)


def turn(x, amount):
    amount = amount % LANES
    return x if amount == 0 else pltpu.roll(x, amount, 1)


def next_col(pair, lane):
    first, second = turn(pair[0], -1), turn(pair[1], -1)
    return jnp.where(lane == LANES - 1, second, first), second


def prev_col(pair, lane):
    first, second = turn(pair[0], 1), turn(pair[1], 1)
    return first, jnp.where(lane == 0, first, second)


def tile(t):
    return pl.ds(t * LANES, LANES)


def row_pair(ref, *index):
    return ref[(*index, slice(None), tile(0))], ref[(*index, slice(None), tile(1))]


def spread(ref, row, plane, t):
    return jnp.broadcast_to(ref[row, pl.ds(plane, 1), tile(t)], (LEVELS, LANES))


def spread_pair(ref, row, plane):
    return spread(ref, row, plane, 0), spread(ref, row, plane, 1)


def both(fn, *pairs):
    return tuple(fn(*(p[t] for p in pairs)) for t in range(2))


def weigh(n0, n1, s0, s1):
    start = n0 / s0
    middle = (n0 + n0 + n1) / (s0 + s0 + s1)
    end = (n0 + n1) / (s0 + s1)
    twice = middle + middle
    late = twice + end
    return (start + twice + late) * (1.0 / 6.0), late * (1.0 / 6.0)


def first_vertex(cor, k0, k1, k2, f0, f1, f2_down, g0, g1, g2_down, h, h_down, h_right, m, m_down, m_right):
    n0 = cor * (k0 + k1 + k2) + (f0 + f2_down - f1)
    n1 = g0 + g2_down - g1
    s0 = k0 * h + k1 * h_down + k2 * h_right
    s1 = k0 * m + k1 * m_down + k2 * m_right
    return weigh(n0, n1, s0, s1)


def second_vertex(cor, k0, k1, k2, f1, f2, f0_diag, g1, g2, g0_diag, h, h_right, h_diag, m, m_right, m_diag):
    n0 = cor * (k0 + k1 + k2) + (f1 - f2 - f0_diag)
    n1 = g1 - g2 - g0_diag
    s0 = k0 * h + k1 * h_right + k2 * h_diag
    s1 = k0 * m + k1 * m_right + k2 * m_diag
    return weigh(n0, n1, s0, s1)


def energy_of(v, w, d, e):
    return (v * (v + w) + (w * w) * (1.0 / 3.0)) * (0.25 * d * e)


def vertices(lo, hi, v, h, w, m, ga, gb, out):
    def flux(ref, k, row):
        return both(lambda a, d: a * d, row_pair(ref, k, row), spread_pair(ga, row, k))

    def right_of(row):
        lane = lane_id()
        return (
            next_col(flux(v, 0, row), lane)
            + next_col(flux(w, 0, row), lane)
            + next_col(row_pair(h, row), lane)
            + next_col(row_pair(m, row), lane)
        )

    def body(row, carry):
        lane = lane_id()
        f0_diag, g0_diag, h_diag, m_diag = (carry[i : i + 2] for i in (0, 2, 4, 6))
        f2, g2, hh, mm = (carry[i : i + 2] for i in (8, 10, 12, 14))
        below = jnp.minimum(row + 1, EXT - 1)
        d0, d1 = spread_pair(ga, row, 0), spread_pair(ga, row, 1)
        mul = lambda a, d: a * d
        f0 = both(mul, row_pair(v, 0, row), d0)
        f1 = both(mul, row_pair(v, 1, row), d1)
        g0 = both(mul, row_pair(w, 0, row), d0)
        g1 = both(mul, row_pair(w, 1, row), d1)
        f2_down, g2_down = flux(v, 2, below), flux(w, 2, below)
        h_down, m_down = row_pair(h, below), row_pair(m, below)
        f0_right, g0_right = next_col(f0, lane), next_col(g0, lane)
        h_right, m_right = next_col(hh, lane), next_col(mm, lane)
        kite = [spread_pair(gb, row, p) for p in range(6)]
        cor0, cor1 = spread_pair(ga, row, 4), spread_pair(ga, row, 5)
        for t in range(2):
            a, b = first_vertex(
                cor0[t], kite[0][t], kite[1][t], kite[2][t], f0[t], f1[t], f2_down[t], g0[t], g1[t], g2_down[t],
                hh[t], h_down[t], h_right[t], mm[t], m_down[t], m_right[t],
            )
            out[0, row, :, tile(t)] = a
            out[1, row, :, tile(t)] = b
            a, b = second_vertex(
                cor1[t], kite[3][t], kite[4][t], kite[5][t], f1[t], f2[t], f0_diag[t], g1[t], g2[t], g0_diag[t],
                hh[t], h_right[t], h_diag[t], mm[t], m_right[t], m_diag[t],
            )
            out[2, row, :, tile(t)] = a
            out[3, row, :, tile(t)] = b
        return f0_right + g0_right + h_right + m_right + f2_down + g2_down + h_down + m_down

    start = right_of(max(lo - 1, 0)) + flux(v, 2, lo) + flux(w, 2, lo) + row_pair(h, lo) + row_pair(m, lo)
    lax.fori_loop(lo, hi, body, start)


def cells(lo, hi, sums, out):
    def body(row, _):
        lane = lane_id()
        for n in range(2):
            v0, v1 = row_pair(sums, n, row), row_pair(sums, 2 + n, row)
            above, below = row_pair(sums, n, row - 1), row_pair(sums, 2 + n, row + 1)
            here = both(lambda a, b: a + b, v0, v1)
            left = prev_col(both(lambda a, b: a + b, here, below), lane)
            for t in range(2):
                out[n, row, :, tile(t)] = (here[t] + above[t] + left[t]) * (1.0 / 6.0)
        return 0

    lax.fori_loop(lo, hi, body, 0)


def energies(lo, hi, v, w, ga, gb, inverse, out):
    spots = ((ga, 6), (ga, 7), (gb, 6))

    def one(k, row):
        ref, plane = spots[k]
        return both(energy_of, row_pair(v, k, row), row_pair(w, k, row), spread_pair(ga, row, k), spread_pair(ref, row, plane))

    def body(row, carry):
        lane = lane_id()
        above, e2 = carry[0:2], carry[2:4]
        e0, e1, e2_down = one(0, row), one(1, row), one(2, row + 1)
        left = prev_col(both(lambda a, b: a + b, e1, e2_down), lane)
        area = spread_pair(inverse, row, 3)
        for t in range(2):
            out[row - 2, :, tile(t)] = (e0[t] + e1[t] + e2[t] + above[t] + left[t]) * area[t]
        return e0 + e2_down

    lax.fori_loop(lo, hi, body, one(0, lo - 1) + one(2, lo))


def exchange_kernel(
    v_in, h_in, w_in, m_in, cd_in, el_in, ca_in, ka_in, co_in,
    v, w, sums, cell, kin, inverse, rim_v, rim_c, rim_k,
    h, m, ga, gb, own, to_right, to_left, from_left, from_right, corner_tr, corner_br, corner_bl, rim,
    load_sem, send_sem, recv_sem,
):
    ny, nx = lax.axis_size("py"), lax.axis_size("px")
    my, mx = lax.axis_index("py"), lax.axis_index("px")

    def device(dy, dx):
        return {"py": lax.rem(my + dy + ny, ny), "px": lax.rem(mx + dx + nx, nx)}

    barrier = pltpu.get_barrier_semaphore()
    for dy, dx in TARGETS:
        pl.semaphore_signal(barrier, inc=1, device_id=device(-dy, -dx), device_id_type=MESH)

    loads = []

    def load(src, dst):
        loads.append(pltpu.make_async_copy(src, dst, load_sem.at[len(loads)]))
        loads[-1].start()

    mine = pl.ds(2, ROWS)
    for p in range(3):
        load(cd_in.at[p], ga.at[mine, p])
    load(ca_in, ga.at[mine, 3])
    for p in range(2):
        load(co_in.at[p], ga.at[mine, 4 + p])
        load(el_in.at[p], ga.at[mine, 6 + p])
    for a in range(2):
        for p in range(3):
            load(ka_in.at[a, p], gb.at[mine, 3 * a + p])
    load(el_in.at[2], gb.at[mine, 6])
    load(el_in.at[2], gb.at[mine, 7])
    for k in range(LEVELS):
        load(h_in.at[k], h.at[mine, k])
        load(m_in.at[k], m.at[mine, k])
        load(v_in.at[:, k], v.at[:, mine, k])
        load(w_in.at[:, k], w.at[:, mine, k])
    for copy in loads:
        copy.wait()

    lane = lane_id()
    slot = lane & 7

    def field(f, row, t):
        if f < 3:
            return v[f, row, :, tile(t)]
        if f < 6:
            return w[f - 3, row, :, tile(t)]
        return (h, m, ga, gb)[f - 6][row, :, tile(t)]

    def strip(f, e):
        return jnp.where(lane >= 64, field(f, e, 1), field(f, e, 0))

    for b in range(3):
        rows = [r for r in range(FIRST[b], FIRST[b] + 16) if 0 <= r < ROWS]
        total = [jnp.zeros((LEVELS, LANES), F32)] * FIELDS
        for r in rows:
            q = (r - FIRST[b]) * 8
            mask = (lane >= q) & (lane < q + 4)
            for f in range(FIELDS):
                total[f] = jnp.where(mask, turn(strip(f, r + 2), q - 126), total[f])
        for f in range(FIELDS):
            own[f, b] = total[f]
        for s in range(2):
            pack = jnp.zeros((LEVELS, LANES), F32)
            for f in range(8 * s, min(8 * s + 8, FIELDS)):
                pack = jnp.where(slot == f - 8 * s, turn(total[f], f - 8 * s - 1), pack)
            to_right[b, s] = pack
        for s in range(3):
            pack = jnp.zeros((LEVELS, LANES), F32)
            for f in range(4 * s, min(4 * s + 4, FIELDS)):
                at = 2 * (f - 4 * s)
                pack = jnp.where((slot == at) | (slot == at + 1), turn(total[f], at - 2), pack)
            to_left[b, s] = pack

    pl.semaphore_wait(barrier, len(TARGETS))

    sends = []

    def send(src, dst, target):
        n = len(sends)
        sends.append(
            pltpu.make_async_remote_copy(
                src_ref=src, dst_ref=dst, send_sem=send_sem.at[n], recv_sem=recv_sem.at[n],
                device_id=device(*target), device_id_type=MESH,
            )
        )
        sends[-1].start()

    top, bottom = pl.ds(0, 2), pl.ds(EXT - 2, 2)
    last, lead = pl.ds(ROWS, 2), pl.ds(2, 2)
    for ref in (v, w):
        send(ref.at[0:2, last], ref.at[0:2, top], DOWN)
        send(ref.at[2, ROWS + 1], ref.at[2, 1], DOWN)
        send(ref.at[1:3, lead], ref.at[1:3, bottom], UP)
        send(ref.at[0, 2], ref.at[0, EXT - 2], UP)
    for ref in (h, m, ga, gb):
        send(ref.at[last], ref.at[top], DOWN)
        send(ref.at[lead], ref.at[bottom], UP)
    send(to_left.at[2], corner_tr, DOWN_LEFT)
    send(to_left.at[0], corner_br, UP_LEFT)
    send(to_right.at[0], corner_bl, UP_RIGHT)
    send(to_right, from_left, RIGHT)
    send(to_left, from_right, LEFT)

    def invert(row, _):
        for t in range(2):
            inverse[row, :, tile(t)] = 1.0 / ga[row, :, tile(t)]
        return 0

    lax.fori_loop(2, ROWS + 2, invert, 0)
    vertices(3, ROWS + 1, v, h, w, m, ga, gb, sums)
    energies(3, ROWS + 1, v, w, ga, gb, inverse, kin)
    cells(4, ROWS, sums, cell)

    for copy in sends:
        copy.wait()

    vertices(0, 3, v, h, w, m, ga, gb, sums)
    vertices(ROWS + 1, EXT, v, h, w, m, ga, gb, sums)
    energies(2, 3, v, w, ga, gb, inverse, kin)
    energies(ROWS + 1, ROWS + 2, v, w, ga, gb, inverse, kin)
    cells(1, 4, sums, cell)
    cells(ROWS, ROWS + 3, sums, cell)

    top_rows, bottom_rows = lane < 16, (lane >= 48) & (lane < 64)
    for b in range(3):
        right = [from_right[b, s] for s in range(3)]
        left = [from_left[b, s] for s in range(2)]
        if b == 0:
            right = [jnp.where(top_rows, turn(corner_tr[s], -32), right[s]) for s in range(3)]
        if b == 2:
            right = [jnp.where(bottom_rows, turn(corner_br[s], 32), right[s]) for s in range(3)]
            left = [jnp.where(bottom_rows, turn(corner_bl[s], 32), left[s]) for s in range(2)]
        for f in range(FIELDS):
            x = own[f, b]
            for r in ((-2, -1) if b == 0 else ((32, 33) if b == 2 else ())):
                q = (r - FIRST[b]) * 8
                x = jnp.where((lane >= q) & (lane < q + 4), turn(strip(f, r + 2), q - 126), x)
            y = turn(right[f // 4], 2 - 2 * (f % 4))
            z = turn(left[f // 8], 4 - f % 8)
            x = jnp.where(slot < 2, x, jnp.where(slot < 4, y, jnp.where(slot == 4, z, turn(x, 3))))
            rim[f, b] = x

    for b in range(3):

        def shift(x, di, dj):
            return turn(x, -(8 * di + dj))

        def geo(f, plane):
            return jnp.broadcast_to(rim[f, b, pl.ds(plane, 1), :], (LEVELS, LANES))

        vv, ww = [rim[k, b] for k in range(3)], [rim[3 + k, b] for k in range(3)]
        hh, mm = rim[6, b], rim[7, b]
        d = [geo(8, k) for k in range(3)]
        f = [vv[k] * d[k] for k in range(3)]
        g = [ww[k] * d[k] for k in range(3)]
        h_right, m_right = shift(hh, 0, 1), shift(mm, 0, 1)
        v0, w0 = first_vertex(
            geo(8, 4), geo(9, 0), geo(9, 1), geo(9, 2), f[0], f[1], shift(f[2], 1, 0), g[0], g[1], shift(g[2], 1, 0),
            hh, shift(hh, 1, 0), h_right, mm, shift(mm, 1, 0), m_right,
        )
        v1, w1 = second_vertex(
            geo(8, 5), geo(9, 3), geo(9, 4), geo(9, 5), f[1], f[2], shift(f[0], -1, 1), g[1], g[2], shift(g[0], -1, 1),
            hh, h_right, shift(hh, -1, 1), mm, m_right, shift(mm, -1, 1),
        )
        rim_v[0, b] = v0
        rim_v[1, b] = v1
        for n, (x0, x1) in enumerate(((v0, v1), (w0, w1))):
            here = x0 + x1
            rim_c[n, b] = (here + shift(x0, -1, 0) + shift(here + shift(x1, 1, 0), 0, -1)) * (1.0 / 6.0)
        length = (geo(8, 6), geo(8, 7), geo(9, 6))
        e = [energy_of(vv[k], ww[k], d[k], length[k]) for k in range(3)]
        rim_k[b] = (e[0] + e[1] + e[2] + shift(e[0], -1, 0) + shift(e[1] + shift(e[2], 1, 0), 0, -1)) / geo(8, 3)


def output_kernel(
    v, w, sums, cell, kin, inverse, rim_v, rim_c, rim_k,
    vertex_out, kinetic_out, cell_out, edge_out,
    vertex_buf, kinetic_buf, cell_buf, edge_buf, sem,
):
    lane = lane_id()
    is_last, is_first = lane == LANES - 1, lane == 0

    def pick(ref, n, row, s, to):
        block, q = rim_of(row)
        x = ref[block] if n is None else ref[n, block]
        return turn(x, to - (q + s))

    def cell_row(n, r):
        first, second = row_pair(cell, n, r + 2)
        if r >= 0 and r <= ROWS:
            first = jnp.where(is_first, pick(rim_c, n, r, 5, 0), first)
        second = jnp.where(is_last, pick(rim_c, n, r, 1, LANES - 1), second)
        return first, second

    def cell_right(n, r, pair):
        first, second = turn(pair[0], -1), turn(pair[1], -1)
        return jnp.where(is_last, second, first), jnp.where(is_last, pick(rim_c, n, r, 2, LANES - 1), second)

    def vertex_row(n, r):
        first, second = row_pair(sums, 2 * n, r + 2)
        return first, jnp.where(is_last, pick(rim_v, n, r, 1, LANES - 1), second)

    copies = []

    def put(src, dst):
        copies.append(pltpu.make_async_copy(src, dst, sem.at[len(copies)]))
        copies[-1].start()

    here = [cell_row(n, 0) for n in range(2)]
    upper_right = [cell_right(n, -1, cell_row(n, -1)) for n in range(2)]
    v0_above, v1 = vertex_row(0, -1), vertex_row(1, 0)
    for r in range(ROWS):
        lower = [cell_row(n, r + 1) for n in range(2)]
        right = [cell_right(n, r, here[n]) for n in range(2)]
        v0, v1_below = vertex_row(0, r), vertex_row(1, r + 1)
        first, second = turn(v1_below[0], 1), turn(v1_below[1], 1)
        v1_corner = (
            jnp.where(is_first, pick(rim_v, 1, r + 1, 4, 0), first),
            jnp.where(is_first, first, second),
        )
        energy = row_pair(kin, r)
        energy = (jnp.where(is_first, pick(rim_k, None, r, 5, 0), energy[0]), energy[1])
        velocity = [row_pair(v, k, r + 2) for k in range(3)]
        tendency = [row_pair(w, k, r + 2) for k in range(3)]
        factor = [spread_pair(inverse, r + 2, k) for k in range(3)]
        for t in range(2):
            vertex_buf[0, r, :, tile(t)] = v0[t]
            vertex_buf[1, r, :, tile(t)] = v1[t]
            kinetic_buf[r, :, tile(t)] = energy[t]
            cell_buf[r, :, tile(t)] = here[0][t]
            means = (v0[t] + v1_corner[t], v0[t] + v1[t], v1[t] + v0_above[t])
            sides = (lower, right, upper_right)
            for k in range(3):
                slope = velocity[k][t] * (sides[k][0][t] - here[0][t]) + tendency[k][t] * (sides[k][1][t] - here[1][t])
                edge_buf[k, r, :, tile(t)] = 0.5 * (means[k] - slope * factor[k][t])
        here, upper_right, v0_above, v1 = lower, right, v0, v1_below
        if r % 16 == 15:
            part = pl.ds(r - 15, 16)
            for k in range(LEVELS):
                put(vertex_buf.at[:, part, k], vertex_out.at[:, k, part])
                put(kinetic_buf.at[part, k], kinetic_out.at[k, part])
                put(cell_buf.at[part, k], cell_out.at[k, part])
                put(edge_buf.at[:, part, k], edge_out.at[:, k, part])
    for copy in copies:
        copy.wait()


def local(*args):
    args = [pltpu.with_memory_space_constraint(x, pltpu.HBM) for x in args]
    whole = pl.BlockSpec(memory_space=pltpu.VMEM)
    anywhere = pl.BlockSpec(memory_space=pl.ANY)
    wide = (LEVELS, 2 * LANES)
    thin = (LEVELS, LANES)
    passed = [
        (3, EXT, *wide), (3, EXT, *wide), (4, EXT, *wide), (2, EXT, *wide), (ROWS, *wide), (EXT, *wide),
        (2, 3, *thin), (2, 3, *thin), (3, *thin),
    ]
    grant = 24 << 20
    between = pl.pallas_call(
        exchange_kernel,
        out_shape=[pltpu.VMEM(s, F32) for s in passed],
        in_specs=[anywhere] * 9,
        out_specs=[whole] * len(passed),
        scratch_shapes=[
            pltpu.VMEM((EXT, *wide), F32), pltpu.VMEM((EXT, *wide), F32),
            pltpu.VMEM((EXT, *wide), F32), pltpu.VMEM((EXT, *wide), F32),
            pltpu.VMEM((FIELDS, 3, *thin), F32),
            pltpu.VMEM((3, 2, *thin), F32), pltpu.VMEM((3, 3, *thin), F32),
            pltpu.VMEM((3, 2, *thin), F32), pltpu.VMEM((3, 3, *thin), F32),
            pltpu.VMEM((3, *thin), F32), pltpu.VMEM((3, *thin), F32), pltpu.VMEM((2, *thin), F32),
            pltpu.VMEM((FIELDS, 3, *thin), F32),
            pltpu.SemaphoreType.DMA((48,)), pltpu.SemaphoreType.DMA((21,)), pltpu.SemaphoreType.DMA((21,)),
        ],
        compiler_params=pltpu.CompilerParams(collective_id=0, has_side_effects=True, vmem_limit_bytes=grant),
    )(*args)
    outs = [(2, LEVELS, ROWS, 2 * LANES), (LEVELS, ROWS, 2 * LANES), (LEVELS, ROWS, 2 * LANES), (3, LEVELS, ROWS, 2 * LANES)]
    return tuple(
        pl.pallas_call(
            output_kernel,
            out_shape=[jax.ShapeDtypeStruct(s, F32) for s in outs],
            in_specs=[whole] * len(passed),
            out_specs=[anywhere] * 4,
            scratch_shapes=[
                pltpu.VMEM((2, ROWS, *wide), F32), pltpu.VMEM((ROWS, *wide), F32),
                pltpu.VMEM((ROWS, *wide), F32), pltpu.VMEM((3, ROWS, *wide), F32),
                pltpu.SemaphoreType.DMA((64,)),
            ],
            compiler_params=pltpu.CompilerParams(vmem_limit_bytes=grant),
        )(*between)
    )


def solution(mesh):
    edges, cell = P(None, None, "py", "px"), P(None, "py", "px")
    return jax.shard_map(
        local,
        mesh=mesh,
        in_specs=(edges, cell, edges, cell, cell, cell, P("py", "px"), edges, cell),
        out_specs=(edges, cell, cell, edges),
        check_vma=False,
    )
```

```python
import jax
import jax.numpy as jnp
from jax import lax
from jax.experimental import pallas as pl
from jax.experimental.pallas import tpu as pltpu
from jax.sharding import PartitionSpec as P

F32 = jnp.float32
MESH = pl.DeviceIdType.MESH
ROWS = 32
EXT = ROWS + 4
LEVELS = 8
LANES = 128

FIRST = (-2, 12, 26)
FIELDS = 10
GROUP = 6

DOWN, UP, RIGHT, LEFT = (1, 0), (-1, 0), (0, 1), (0, -1)
DOWN_LEFT, UP_LEFT, UP_RIGHT = (1, -1), (-1, -1), (-1, 1)
TARGETS = (DOWN, UP, RIGHT, LEFT, DOWN_LEFT, UP_LEFT, UP_RIGHT)


def rim_of(row):
    block = 0 if row <= 12 else (1 if row <= 26 else 2)
    return block, (row - FIRST[block]) * 8


def lane_id():
    return lax.broadcasted_iota(jnp.int32, (LEVELS, LANES), 1)


def turn(x, amount):
    amount = amount % LANES
    return x if amount == 0 else pltpu.roll(x, amount, 1)


def next_col(pair, lane):
    first, second = turn(pair[0], -1), turn(pair[1], -1)
    return jnp.where(lane == LANES - 1, second, first), second


def prev_col(pair, lane):
    first, second = turn(pair[0], 1), turn(pair[1], 1)
    return first, jnp.where(lane == 0, first, second)


def tile(t):
    return pl.ds(t * LANES, LANES)


def row_pair(ref, *index):
    return ref[(*index, slice(None), tile(0))], ref[(*index, slice(None), tile(1))]


def spread(ref, row, plane, t):
    return jnp.broadcast_to(ref[row, pl.ds(plane, 1), tile(t)], (LEVELS, LANES))


def spread_pair(ref, row, plane):
    return spread(ref, row, plane, 0), spread(ref, row, plane, 1)


def both(fn, *pairs):
    return tuple(fn(*(p[t] for p in pairs)) for t in range(2))


def add(a, b):
    return a + b


def mul(a, b):
    return a * b


def staged(rows, begin, finish, depth):
    waiting = []
    for row in rows:
        waiting.append((row, begin(row)))
        if len(waiting) > depth:
            finish(*waiting.pop(0))
    for row, value in waiting:
        finish(row, value)


def weigh(n0, n1, s0, s1):
    start = n0 / s0
    middle = (n0 + n0 + n1) / (s0 + s0 + s1)
    end = (n0 + n1) / (s0 + s1)
    twice = middle + middle
    late = twice + end
    return (start + twice + late) * (1.0 / 6.0), late * (1.0 / 6.0)


def first_vertex(cor, k0, k1, k2, f0, f1, f2_down, g0, g1, g2_down, h, h_down, h_right, m, m_down, m_right):
    n0 = cor * (k0 + k1 + k2) + (f0 + f2_down - f1)
    n1 = g0 + g2_down - g1
    s0 = k0 * h + k1 * h_down + k2 * h_right
    s1 = k0 * m + k1 * m_down + k2 * m_right
    return weigh(n0, n1, s0, s1)


def second_vertex(cor, k0, k1, k2, f1, f2, f0_diag, g1, g2, g0_diag, h, h_right, h_diag, m, m_right, m_diag):
    n0 = cor * (k0 + k1 + k2) + (f1 - f2 - f0_diag)
    n1 = g1 - g2 - g0_diag
    s0 = k0 * h + k1 * h_right + k2 * h_diag
    s1 = k0 * m + k1 * m_right + k2 * m_diag
    return weigh(n0, n1, s0, s1)


def energy_of(v, w, d, e):
    return (v * (v + w) + (w * w) * (1.0 / 3.0)) * (0.25 * d * e)


def turned_rows(rows, v, h, w, m, ga, right):
    def begin(row):
        d0 = spread_pair(ga, row, 0)
        pairs = (both(mul, row_pair(v, 0, row), d0), both(mul, row_pair(w, 0, row), d0), row_pair(h, row), row_pair(m, row))
        return [(turn(p[0], -1), turn(p[1], -1)) for p in pairs]

    def finish(row, turned):
        last = lane_id() == LANES - 1
        for n, (first, second) in enumerate(turned):
            right[n, row, :, tile(0)] = jnp.where(last, second, first)
            right[n, row, :, tile(1)] = second

    staged(rows, begin, finish, 8)


def vertex_rows(rows, v, h, w, m, ga, gb, right, out, depth=2, skip_first=None, skip_second=None):
    known = {}

    def flux(ref, name, k, row, key):
        if (name, k, key) not in known:
            known[name, k, key] = both(mul, row_pair(ref, k, row), spread_pair(ga, row, k))
        return known[name, k, key]

    def begin(item):
        key, row = item
        f = [flux(v, "v", k, row, key) for k in range(3)]
        g = [flux(w, "w", k, row, key) for k in range(3)]
        hh, mm = row_pair(h, row), row_pair(m, row)
        h_right, m_right = row_pair(right, 2, row), row_pair(right, 3, row)
        results = []
        if key != skip_first:
            below = row + 1
            f2_down, g2_down = flux(v, "v", 2, below, key + 1), flux(w, "w", 2, below, key + 1)
            h_down, m_down = row_pair(h, below), row_pair(m, below)
            cor = spread_pair(ga, row, 4)
            kite = [spread_pair(gb, row, p) for p in range(3)]
            for t in range(2):
                pair = first_vertex(
                    cor[t], kite[0][t], kite[1][t], kite[2][t], f[0][t], f[1][t], f2_down[t], g[0][t], g[1][t],
                    g2_down[t], hh[t], h_down[t], h_right[t], mm[t], m_down[t], m_right[t],
                )
                results += [(0, t, pair[0]), (1, t, pair[1])]
        if key != skip_second:
            above = row - 1
            f0_diag, g0_diag, h_diag, m_diag = (row_pair(right, n, above) for n in range(4))
            cor = spread_pair(ga, row, 5)
            kite = [spread_pair(gb, row, p) for p in range(3, 6)]
            for t in range(2):
                pair = second_vertex(
                    cor[t], kite[0][t], kite[1][t], kite[2][t], f[1][t], f[2][t], f0_diag[t], g[1][t], g[2][t],
                    g0_diag[t], hh[t], h_right[t], h_diag[t], mm[t], m_right[t], m_diag[t],
                )
                results += [(2, t, pair[0]), (3, t, pair[1])]
        return results

    def finish(item, results):
        for n, t, value in results:
            out[n, item[1], :, tile(t)] = value

    staged(rows, begin, finish, depth)


def cell_rows(rows, sums, out):
    def begin(row):
        values = []
        for n in range(2):
            v0, v1 = row_pair(sums, n, row), row_pair(sums, 2 + n, row)
            above, below = row_pair(sums, n, row - 1), row_pair(sums, 2 + n, row + 1)
            here = both(add, v0, v1)
            west = both(add, here, below)
            values.append((both(add, here, above), (turn(west[0], 1), turn(west[1], 1))))
        return values

    def finish(row, values):
        start = lane_id() == 0
        for n, (near, west) in enumerate(values):
            out[n, row, :, tile(0)] = (near[0] + west[0]) * (1.0 / 6.0)
            out[n, row, :, tile(1)] = (near[1] + jnp.where(start, west[0], west[1])) * (1.0 / 6.0)

    staged(rows, begin, finish, 5)


def energy_rows(rows, v, w, ga, gb, inverse, out):
    spots = ((ga, 6), (ga, 7), (gb, 6))
    known = {}

    def one(k, row):
        if (k, row) not in known:
            ref, plane = spots[k]
            known[k, row] = both(
                energy_of, row_pair(v, k, row), row_pair(w, k, row), spread_pair(ga, row, k), spread_pair(ref, row, plane)
            )
        return known[k, row]

    def begin(row):
        e1 = one(1, row)
        near = both(lambda a, b, c, d: a + b + (c + d), one(0, row), one(0, row - 1), e1, one(2, row))
        west = both(add, e1, one(2, row + 1))
        return near, (turn(west[0], 1), turn(west[1], 1))

    def finish(row, values):
        near, west = values
        start = lane_id() == 0
        area = spread_pair(inverse, row, 3)
        out[row - 2, :, tile(0)] = (near[0] + west[0]) * area[0]
        out[row - 2, :, tile(1)] = (near[1] + jnp.where(start, west[0], west[1])) * area[1]

    staged(rows, begin, finish, 6)


def exchange_kernel(
    v_in, h_in, w_in, m_in, cd_in, el_in, ca_in, ka_in, co_in,
    v, w, sums, cell, kin, inverse, rim_patch, rim_c, rim_right,
    h, m, ga, gb, turned, own, to_right, to_left, from_left, from_right, corner_tr, corner_br, corner_bl, rim,
    load_sem, send_sem, recv_sem,
):
    ny, nx = lax.axis_size("py"), lax.axis_size("px")
    my, mx = lax.axis_index("py"), lax.axis_index("px")

    def device(dy, dx):
        return {"py": lax.rem(my + dy + ny, ny), "px": lax.rem(mx + dx + nx, nx)}

    barrier = pltpu.get_barrier_semaphore()
    for dy, dx in TARGETS:
        pl.semaphore_signal(barrier, inc=1, device_id=device(-dy, -dx), device_id_type=MESH)

    loads = []

    def load(src, dst):
        loads.append(pltpu.make_async_copy(src, dst, load_sem.at[len(loads)]))
        loads[-1].start()

    mine = pl.ds(2, ROWS)
    for k in range(LEVELS):
        load(v_in.at[:, k], v.at[:, mine, k])
        load(w_in.at[:, k], w.at[:, mine, k])
        load(h_in.at[k], h.at[mine, k])
        load(m_in.at[k], m.at[mine, k])
    for p in range(3):
        load(cd_in.at[p], ga.at[mine, p])
    load(ca_in, ga.at[mine, 3])
    for p in range(2):
        load(co_in.at[p], ga.at[mine, 4 + p])
        load(el_in.at[p], ga.at[mine, 6 + p])
    for a in range(2):
        for p in range(3):
            load(ka_in.at[a, p], gb.at[mine, 3 * a + p])
    load(el_in.at[2], gb.at[mine, 6])
    load(el_in.at[2], gb.at[mine, 7])
    for copy in loads:
        copy.wait()

    lane = lane_id()
    slot = lane & 7

    def field(f, row, t):
        if f < 3:
            return v[f, row, :, tile(t)]
        if f < 6:
            return w[f - 3, row, :, tile(t)]
        return (h, m, ga, gb)[f - 6][row, :, tile(t)]

    def strip(f, e):
        return jnp.where(lane >= 64, field(f, e, 1), field(f, e, 0))

    total = {}
    for b in range(3):
        rows = [r for r in range(FIRST[b], FIRST[b] + 16) if 0 <= r < ROWS]
        masks = [(lane >= (r - FIRST[b]) * 8) & (lane < (r - FIRST[b]) * 8 + 4) for r in rows]
        for f in range(FIELDS):
            x = jnp.zeros((LEVELS, LANES), F32)
            for r, mask in zip(rows, masks):
                x = jnp.where(mask, turn(strip(f, r + 2), (r - FIRST[b]) * 8 - 126), x)
            total[f, b] = x
    packs = {}
    for b in range(3):
        for s in range(2):
            x = jnp.zeros((LEVELS, LANES), F32)
            for f in range(8 * s, min(8 * s + 8, FIELDS)):
                x = jnp.where(slot == f - 8 * s, turn(total[f, b], f - 8 * s - 1), x)
            packs[0, b, s] = x
        for s in range(3):
            x = jnp.zeros((LEVELS, LANES), F32)
            for f in range(4 * s, min(4 * s + 4, FIELDS)):
                at = 2 * (f - 4 * s)
                x = jnp.where((slot >> 1) == f - 4 * s, turn(total[f, b], at - 2), x)
            packs[1, b, s] = x
    for (n, b, s), x in packs.items():
        (to_right, to_left)[n][b, s] = x
    for (f, b), x in total.items():
        own[f, b] = x

    pl.semaphore_wait(barrier, len(TARGETS))

    sends = []

    def send(src, dst, target):
        n = len(sends)
        sends.append(
            pltpu.make_async_remote_copy(
                src_ref=src, dst_ref=dst, send_sem=send_sem.at[n], recv_sem=recv_sem.at[n],
                device_id=device(*target), device_id_type=MESH,
            )
        )
        sends[-1].start()

    top, bottom = pl.ds(0, 2), pl.ds(EXT - 2, 2)
    last, lead = pl.ds(ROWS, 2), pl.ds(2, 2)
    for ref in (v, w):
        send(ref.at[0:2, last], ref.at[0:2, top], DOWN)
        send(ref.at[2, ROWS + 1], ref.at[2, 1], DOWN)
        send(ref.at[1:3, lead], ref.at[1:3, bottom], UP)
        send(ref.at[0, 2], ref.at[0, EXT - 2], UP)
    for ref in (h, m, ga, gb):
        send(ref.at[last], ref.at[top], DOWN)
        send(ref.at[lead], ref.at[bottom], UP)
    send(to_left.at[2], corner_tr, DOWN_LEFT)
    send(to_left.at[0], corner_br, UP_LEFT)
    send(to_right.at[0], corner_bl, UP_RIGHT)
    send(to_right, from_left, RIGHT)
    send(to_left, from_right, LEFT)

    def invert(row):
        return [1.0 / ga[row, :, tile(t)] for t in range(2)]

    def keep(row, values):
        for t in range(2):
            inverse[row, :, tile(t)] = values[t]

    staged(range(2, ROWS + 2), invert, keep, 8)
    turned_rows(range(2, ROWS + 2), v, h, w, m, ga, turned)
    energy_rows(range(3, ROWS + 1), v, w, ga, gb, inverse, kin)

    def group(index, _):
        base = 3 + index * GROUP
        vertex_rows([(j, base + j) for j in range(GROUP)], v, h, w, m, ga, gb, turned, sums)
        return 0

    lax.fori_loop(0, (ROWS - 2) // GROUP, group, 0)
    cell_rows(range(4, ROWS), sums, cell)

    for copy in sends:
        copy.wait()

    top_rows, bottom_rows = lane < 16, (lane >= 48) & (lane < 64)
    strips = {}
    for b in range(3):
        right = [from_right[b, s] for s in range(3)]
        left = [from_left[b, s] for s in range(2)]
        if b == 0:
            right = [jnp.where(top_rows, turn(corner_tr[s], -32), right[s]) for s in range(3)]
        if b == 2:
            right = [jnp.where(bottom_rows, turn(corner_br[s], 32), right[s]) for s in range(3)]
            left = [jnp.where(bottom_rows, turn(corner_bl[s], 32), left[s]) for s in range(2)]
        for f in range(FIELDS):
            x = own[f, b]
            for r in ((-2, -1) if b == 0 else ((32, 33) if b == 2 else ())):
                q = (r - FIRST[b]) * 8
                x = jnp.where((lane >= q) & (lane < q + 4), turn(strip(f, r + 2), q - 126), x)
            y = turn(right[f // 4], 2 - 2 * (f % 4))
            z = turn(left[f // 8], 4 - f % 8)
            strips[f, b] = jnp.where(slot < 2, x, jnp.where(slot < 4, y, jnp.where(slot == 4, z, turn(x, 3))))
    turned_rows((0, 1, EXT - 2, EXT - 1), v, h, w, m, ga, turned)
    for (f, b), x in strips.items():
        rim[f, b] = x

    results = {}

    def shift(x, di, dj):
        return turn(x, -(8 * di + dj))

    for b in range(3):

        def geo(f, plane):
            return jnp.broadcast_to(rim[f, b, pl.ds(plane, 1), :], (LEVELS, LANES))

        vv, ww = [rim[k, b] for k in range(3)], [rim[3 + k, b] for k in range(3)]
        hh, mm = rim[6, b], rim[7, b]
        d = [geo(8, k) for k in range(3)]
        f = [vv[k] * d[k] for k in range(3)]
        g = [ww[k] * d[k] for k in range(3)]
        h_right, m_right = shift(hh, 0, 1), shift(mm, 0, 1)
        v0, w0 = first_vertex(
            geo(8, 4), geo(9, 0), geo(9, 1), geo(9, 2), f[0], f[1], shift(f[2], 1, 0), g[0], g[1], shift(g[2], 1, 0),
            hh, shift(hh, 1, 0), h_right, mm, shift(mm, 1, 0), m_right,
        )
        v1, w1 = second_vertex(
            geo(8, 5), geo(9, 3), geo(9, 4), geo(9, 5), f[1], f[2], shift(f[0], -1, 1), g[1], g[2], shift(g[0], -1, 1),
            hh, h_right, shift(hh, -1, 1), mm, m_right, shift(mm, -1, 1),
        )
        length = (geo(8, 6), geo(8, 7), geo(9, 6))
        e = [energy_of(vv[k], ww[k], d[k], length[k]) for k in range(3)]
        energy = (e[0] + e[1] + e[2] + shift(e[0], -1, 0) + (shift(e[1], 0, -1) + shift(e[2], 1, -1))) / geo(8, 3)
        results[0, 0, b] = jnp.where(slot == 0, shift(v0, 0, 1), shift(energy, 0, 4))
        results[0, 1, b] = jnp.where(slot == 0, shift(v1, 0, 1), shift(v1, 1, 3))
        for n, (x0, x1) in enumerate(((v0, v1), (w0, w1))):
            here = x0 + x1
            mean = (here + shift(x0, -1, 0) + (shift(here, 0, -1) + shift(x1, 1, -1))) * (1.0 / 6.0)
            results[1, n, b] = jnp.where(slot == 0, shift(mean, 0, 1), shift(mean, 0, 4))
            results[2, n, b] = mean
    for (which, n, b), x in results.items():
        (rim_patch, rim_c, rim_right)[which][n, b] = x

    vertex_rows([(e, e) for e in (0, 1, 2, ROWS + 1, ROWS + 2, ROWS + 3)], v, h, w, m, ga, gb, turned, sums, 2, EXT - 1, 0)
    energy_rows((2, ROWS + 1), v, w, ga, gb, inverse, kin)
    cell_rows((1, 2, 3, ROWS, ROWS + 1, ROWS + 2), sums, cell)


def output_kernel(
    v, w, sums, cell, kin, inverse, rim_patch, rim_c, rim_right,
    vertex_out, kinetic_out, cell_out, edge_out,
    vertex_buf, kinetic_buf, cell_buf, edge_buf, other_buf, right_buf, corner_buf, sem,
):
    lane = lane_id()
    is_last, is_first, tail = lane == LANES - 1, lane == 0, lane >= LANES - 2

    def pick(ref, n, row, s, to):
        block, q = rim_of(row)
        return turn(ref[n, block], to - (q + s))

    copies = []

    def put(src, dst):
        copies.append(pltpu.make_async_copy(src, dst, sem.at[len(copies)]))
        copies[-1].start()

    def begin(r):
        values = []
        for n in range(2):
            pair = row_pair(cell, n, r + 2)
            values += [pair, turn(pair[0], -1), turn(pair[1], -1), pick(rim_c, n, r, 0, LANES - 1), pick(rim_right, n, r, 1, LANES - 2)]
        if r < ROWS:
            values += [row_pair(sums, 0, r + 2), pick(rim_patch, 0, r, 0, LANES - 1)]
            if r >= 0:
                values += [row_pair(sums, 2, r + 2), row_pair(kin, r), pick(rim_patch, 1, r, 0, LANES - 1)]
                below = row_pair(sums, 2, r + 3)
                values += [turn(below[0], 1), turn(below[1], 1)]
        return values

    def finish(r, values):
        for n, buf in ((0, cell_buf), (1, other_buf)):
            pair, first, second, patch, patch_right = values[5 * n : 5 * n + 5]
            buf[r + 1, :, tile(0)] = jnp.where(is_first, patch, pair[0])
            buf[r + 1, :, tile(1)] = jnp.where(is_last, patch, pair[1])
            right_buf[n, r + 1, :, tile(0)] = jnp.where(is_last, second, first)
            right_buf[n, r + 1, :, tile(1)] = jnp.where(tail, patch_right, second)
        if r < ROWS:
            v0, patch = values[10:12]
            vertex_buf[0, r + 1, :, tile(0)] = v0[0]
            vertex_buf[0, r + 1, :, tile(1)] = jnp.where(is_last, patch, v0[1])
            if r >= 0:
                v1, energy, other, first, second = values[12:17]
                kinetic_buf[r, :, tile(0)] = jnp.where(is_first, patch, energy[0])
                kinetic_buf[r, :, tile(1)] = energy[1]
                vertex_buf[1, r + 1, :, tile(0)] = v1[0]
                vertex_buf[1, r + 1, :, tile(1)] = jnp.where(is_last, other, v1[1])
                corner_buf[r, :, tile(0)] = jnp.where(is_first, other, first)
                corner_buf[r, :, tile(1)] = jnp.where(is_first, first, second)

    staged(range(-1, ROWS + 1), begin, finish, 8)
    for k in range(LEVELS):
        put(vertex_buf.at[:, 1 : ROWS + 1, k], vertex_out.at[:, k])
        put(kinetic_buf.at[:, k], kinetic_out.at[k])
        put(cell_buf.at[1 : ROWS + 1, k], cell_out.at[k])

    def slopes(r):
        v0, v1 = row_pair(vertex_buf, 0, r + 1), row_pair(vertex_buf, 1, r + 1)
        means = (
            both(add, v0, row_pair(corner_buf, r)),
            both(add, v0, v1),
            both(add, v1, row_pair(vertex_buf, 0, r)),
        )
        here = (row_pair(cell_buf, r + 1), row_pair(other_buf, r + 1))
        lower = (row_pair(cell_buf, r + 2), row_pair(other_buf, r + 2))
        right = (row_pair(right_buf, 0, r + 1), row_pair(right_buf, 1, r + 1))
        upper = (row_pair(right_buf, 0, r), row_pair(right_buf, 1, r))
        values = []
        for k, side in enumerate((lower, right, upper)):
            velocity, tendency = row_pair(v, k, r + 2), row_pair(w, k, r + 2)
            factor = spread_pair(inverse, r + 2, k)
            for t in range(2):
                slope = velocity[t] * (side[0][t] - here[0][t]) + tendency[t] * (side[1][t] - here[1][t])
                values.append(0.5 * (means[k][t] - slope * factor[t]))
        return values

    def keep(r, values):
        for k in range(3):
            for t in range(2):
                edge_buf[k, r, :, tile(t)] = values[2 * k + t]

    half = ROWS // 2
    for part in range(2):
        rows = pl.ds(part * half, half)
        staged(range(part * half, (part + 1) * half), slopes, keep, 3)
        for k in range(LEVELS):
            put(edge_buf.at[:, rows, k], edge_out.at[:, k, rows])
    for copy in copies:
        copy.wait()


def local(*args):
    args = [pltpu.with_memory_space_constraint(x, pltpu.HBM) for x in args]
    whole = pl.BlockSpec(memory_space=pltpu.VMEM)
    anywhere = pl.BlockSpec(memory_space=pl.ANY)
    wide = (LEVELS, 2 * LANES)
    thin = (LEVELS, LANES)
    passed = [
        (3, EXT, *wide), (3, EXT, *wide), (4, EXT, *wide), (2, EXT, *wide), (ROWS, *wide), (EXT, *wide),
        (2, 3, *thin), (2, 3, *thin), (2, 3, *thin),
    ]
    grant = 24 << 20
    between = pl.pallas_call(
        exchange_kernel,
        out_shape=[pltpu.VMEM(s, F32) for s in passed],
        in_specs=[anywhere] * 9,
        out_specs=[whole] * len(passed),
        scratch_shapes=[
            pltpu.VMEM((EXT, *wide), F32), pltpu.VMEM((EXT, *wide), F32),
            pltpu.VMEM((EXT, *wide), F32), pltpu.VMEM((EXT, *wide), F32),
            pltpu.VMEM((4, EXT, *wide), F32), pltpu.VMEM((FIELDS, 3, *thin), F32),
            pltpu.VMEM((3, 2, *thin), F32), pltpu.VMEM((3, 3, *thin), F32),
            pltpu.VMEM((3, 2, *thin), F32), pltpu.VMEM((3, 3, *thin), F32),
            pltpu.VMEM((3, *thin), F32), pltpu.VMEM((3, *thin), F32), pltpu.VMEM((2, *thin), F32),
            pltpu.VMEM((FIELDS, 3, *thin), F32),
            pltpu.SemaphoreType.DMA((48,)), pltpu.SemaphoreType.DMA((21,)), pltpu.SemaphoreType.DMA((21,)),
        ],
        compiler_params=pltpu.CompilerParams(collective_id=0, has_side_effects=True, vmem_limit_bytes=grant),
    )(*args)
    outs = [(2, LEVELS, ROWS, 2 * LANES), (LEVELS, ROWS, 2 * LANES), (LEVELS, ROWS, 2 * LANES), (3, LEVELS, ROWS, 2 * LANES)]
    return tuple(
        pl.pallas_call(
            output_kernel,
            out_shape=[jax.ShapeDtypeStruct(s, F32) for s in outs],
            in_specs=[whole] * len(passed),
            out_specs=[anywhere] * 4,
            scratch_shapes=[
                pltpu.VMEM((2, ROWS + 1, *wide), F32), pltpu.VMEM((ROWS, *wide), F32),
                pltpu.VMEM((ROWS + 2, *wide), F32), pltpu.VMEM((3, ROWS, *wide), F32),
                pltpu.VMEM((ROWS + 2, *wide), F32), pltpu.VMEM((2, ROWS + 2, *wide), F32), pltpu.VMEM((ROWS, *wide), F32),
                pltpu.SemaphoreType.DMA((64,)),
            ],
            compiler_params=pltpu.CompilerParams(vmem_limit_bytes=grant),
        )(*between)
    )


def solution(mesh):
    edges, cell = P(None, None, "py", "px"), P(None, "py", "px")
    return jax.shard_map(
        local,
        mesh=mesh,
        in_specs=(edges, cell, edges, cell, cell, cell, P("py", "px"), edges, cell),
        out_specs=(edges, cell, cell, edges),
        check_vma=False,
    )
```

```python
import jax
import jax.numpy as jnp
from jax import lax
from jax.experimental import pallas as pl
from jax.experimental.pallas import tpu as pltpu
from jax.sharding import PartitionSpec as P

F32 = jnp.float32
MESH = pl.DeviceIdType.MESH
ROWS = 32
EXT = ROWS + 4
LEVELS = 8
LANES = 128

FIRST = (-2, 12, 26)
FIELDS = 10
GROUP = 6

DOWN, UP, RIGHT, LEFT = (1, 0), (-1, 0), (0, 1), (0, -1)
DOWN_LEFT, UP_LEFT, UP_RIGHT = (1, -1), (-1, -1), (-1, 1)
TARGETS = (DOWN, UP, RIGHT, LEFT, DOWN_LEFT, UP_RIGHT)


def rim_of(row):
    block = 0 if row <= 12 else (1 if row <= 26 else 2)
    return block, (row - FIRST[block]) * 8


def lane_id():
    return lax.broadcasted_iota(jnp.int32, (LEVELS, LANES), 1)


def turn(x, amount):
    amount = amount % LANES
    return x if amount == 0 else pltpu.roll(x, amount, 1)


def next_col(pair, lane):
    first, second = turn(pair[0], -1), turn(pair[1], -1)
    return jnp.where(lane == LANES - 1, second, first), second


def prev_col(pair, lane):
    first, second = turn(pair[0], 1), turn(pair[1], 1)
    return first, jnp.where(lane == 0, first, second)


def tile(t):
    return pl.ds(t * LANES, LANES)


def row_pair(ref, *index):
    return ref[(*index, slice(None), tile(0))], ref[(*index, slice(None), tile(1))]


def spread(ref, row, plane, t):
    return jnp.broadcast_to(ref[row, pl.ds(plane, 1), tile(t)], (LEVELS, LANES))


def spread_pair(ref, row, plane):
    return spread(ref, row, plane, 0), spread(ref, row, plane, 1)


def both(fn, *pairs):
    return tuple(fn(*(p[t] for p in pairs)) for t in range(2))


def add(a, b):
    return a + b


def mul(a, b):
    return a * b


def staged(rows, begin, finish, depth):
    waiting = []
    for row in rows:
        waiting.append((row, begin(row)))
        if len(waiting) > depth:
            finish(*waiting.pop(0))
    for row, value in waiting:
        finish(row, value)


def weigh(n0, n1, s0, s1):
    start = n0 / s0
    middle = (n0 + n0 + n1) / (s0 + s0 + s1)
    end = (n0 + n1) / (s0 + s1)
    twice = middle + middle
    late = twice + end
    return (start + twice + late) * (1.0 / 6.0), late * (1.0 / 6.0)


def first_vertex(cor, k0, k1, k2, f0, f1, f2_down, g0, g1, g2_down, h, h_down, h_right, m, m_down, m_right):
    n0 = cor * (k0 + k1 + k2) + (f0 + f2_down - f1)
    n1 = g0 + g2_down - g1
    s0 = k0 * h + k1 * h_down + k2 * h_right
    s1 = k0 * m + k1 * m_down + k2 * m_right
    return weigh(n0, n1, s0, s1)


def second_vertex(cor, k0, k1, k2, f1, f2, f0_diag, g1, g2, g0_diag, h, h_right, h_diag, m, m_right, m_diag):
    n0 = cor * (k0 + k1 + k2) + (f1 - f2 - f0_diag)
    n1 = g1 - g2 - g0_diag
    s0 = k0 * h + k1 * h_right + k2 * h_diag
    s1 = k0 * m + k1 * m_right + k2 * m_diag
    return weigh(n0, n1, s0, s1)


def energy_of(v, w, d, e):
    return (v * (v + w) + (w * w) * (1.0 / 3.0)) * (0.25 * d * e)


def turned_rows(rows, v, h, w, m, ga, right):
    def begin(row):
        d0 = spread_pair(ga, row, 0)
        pairs = (both(mul, row_pair(v, 0, row), d0), both(mul, row_pair(w, 0, row), d0), row_pair(h, row), row_pair(m, row))
        return [(turn(p[0], -1), turn(p[1], -1)) for p in pairs]

    def finish(row, turned):
        last = lane_id() == LANES - 1
        for n, (first, second) in enumerate(turned):
            right[n, row, :, tile(0)] = jnp.where(last, second, first)
            right[n, row, :, tile(1)] = second

    staged(rows, begin, finish, 8)


def vertex_rows(rows, v, h, w, m, ga, gb, right, out, depth=2, skip_first=None, skip_second=None):
    known = {}

    def flux(ref, name, k, row, key):
        if (name, k, key) not in known:
            known[name, k, key] = both(mul, row_pair(ref, k, row), spread_pair(ga, row, k))
        return known[name, k, key]

    def begin(item):
        key, row = item
        f = [flux(v, "v", k, row, key) for k in range(3)]
        g = [flux(w, "w", k, row, key) for k in range(3)]
        hh, mm = row_pair(h, row), row_pair(m, row)
        h_right, m_right = row_pair(right, 2, row), row_pair(right, 3, row)
        results = []
        if key != skip_first:
            below = row + 1
            f2_down, g2_down = flux(v, "v", 2, below, key + 1), flux(w, "w", 2, below, key + 1)
            h_down, m_down = row_pair(h, below), row_pair(m, below)
            cor = spread_pair(ga, row, 4)
            kite = [spread_pair(gb, row, p) for p in range(3)]
            for t in range(2):
                pair = first_vertex(
                    cor[t], kite[0][t], kite[1][t], kite[2][t], f[0][t], f[1][t], f2_down[t], g[0][t], g[1][t],
                    g2_down[t], hh[t], h_down[t], h_right[t], mm[t], m_down[t], m_right[t],
                )
                results += [(0, t, pair[0]), (1, t, pair[1])]
        if key != skip_second:
            above = row - 1
            f0_diag, g0_diag, h_diag, m_diag = (row_pair(right, n, above) for n in range(4))
            cor = spread_pair(ga, row, 5)
            kite = [spread_pair(gb, row, p) for p in range(3, 6)]
            for t in range(2):
                pair = second_vertex(
                    cor[t], kite[0][t], kite[1][t], kite[2][t], f[1][t], f[2][t], f0_diag[t], g[1][t], g[2][t],
                    g0_diag[t], hh[t], h_right[t], h_diag[t], mm[t], m_right[t], m_diag[t],
                )
                results += [(2, t, pair[0]), (3, t, pair[1])]
        return results

    def finish(item, results):
        for n, t, value in results:
            out[n, item[1], :, tile(t)] = value

    staged(rows, begin, finish, depth)


def cell_rows(rows, sums, out):
    def begin(row):
        values = []
        for n in range(2):
            v0, v1 = row_pair(sums, n, row), row_pair(sums, 2 + n, row)
            above, below = row_pair(sums, n, row - 1), row_pair(sums, 2 + n, row + 1)
            here = both(add, v0, v1)
            west = both(add, here, below)
            values.append((both(add, here, above), (turn(west[0], 1), turn(west[1], 1))))
        return values

    def finish(row, values):
        start = lane_id() == 0
        for n, (near, west) in enumerate(values):
            out[n, row, :, tile(0)] = (near[0] + west[0]) * (1.0 / 6.0)
            out[n, row, :, tile(1)] = (near[1] + jnp.where(start, west[0], west[1])) * (1.0 / 6.0)

    staged(rows, begin, finish, 5)


def energy_rows(rows, v, w, ga, gb, inverse, out):
    spots = ((ga, 6), (ga, 7), (gb, 6))
    known = {}

    def one(k, row):
        if (k, row) not in known:
            ref, plane = spots[k]
            known[k, row] = both(
                energy_of, row_pair(v, k, row), row_pair(w, k, row), spread_pair(ga, row, k), spread_pair(ref, row, plane)
            )
        return known[k, row]

    def begin(row):
        e1 = one(1, row)
        near = both(lambda a, b, c, d: a + b + (c + d), one(0, row), one(0, row - 1), e1, one(2, row))
        west = both(add, e1, one(2, row + 1))
        return near, (turn(west[0], 1), turn(west[1], 1))

    def finish(row, values):
        near, west = values
        start = lane_id() == 0
        area = spread_pair(inverse, row, 3)
        out[row - 2, :, tile(0)] = (near[0] + west[0]) * area[0]
        out[row - 2, :, tile(1)] = (near[1] + jnp.where(start, west[0], west[1])) * area[1]

    staged(rows, begin, finish, 6)


def exchange_kernel(
    v_in, h_in, w_in, m_in, cd_in, el_in, ca_in, ka_in, co_in,
    v, w, sums, cell, kin, inverse, rim_patch, rim_c, rim_right,
    h, m, ga, gb, turned, own, to_right, to_left, from_left, from_right, corner_tr, corner_br, corner_bl, rim,
    load_sem, send_sem, recv_sem, corner_sem,
):
    ny, nx = lax.axis_size("py"), lax.axis_size("px")
    my, mx = lax.axis_index("py"), lax.axis_index("px")

    def device(dy, dx):
        return {"py": lax.rem(my + dy + ny, ny), "px": lax.rem(mx + dx + nx, nx)}

    barrier = pltpu.get_barrier_semaphore()
    for dy, dx in TARGETS:
        pl.semaphore_signal(barrier, inc=1, device_id=device(-dy, -dx), device_id_type=MESH)

    loads = []

    def load(src, dst):
        loads.append(pltpu.make_async_copy(src, dst, load_sem.at[len(loads)]))
        loads[-1].start()

    mine = pl.ds(2, ROWS)
    for k in range(LEVELS):
        load(v_in.at[:, k], v.at[:, mine, k])
        load(w_in.at[:, k], w.at[:, mine, k])
        load(h_in.at[k], h.at[mine, k])
        load(m_in.at[k], m.at[mine, k])
    for p in range(3):
        load(cd_in.at[p], ga.at[mine, p])
    load(ca_in, ga.at[mine, 3])
    for p in range(2):
        load(co_in.at[p], ga.at[mine, 4 + p])
        load(el_in.at[p], ga.at[mine, 6 + p])
    for a in range(2):
        for p in range(3):
            load(ka_in.at[a, p], gb.at[mine, 3 * a + p])
    load(el_in.at[2], gb.at[mine, 6])
    load(el_in.at[2], gb.at[mine, 7])
    for copy in loads:
        copy.wait()

    lane = lane_id()
    slot = lane & 7

    def field(f, row, t):
        if f < 3:
            return v[f, row, :, tile(t)]
        if f < 6:
            return w[f - 3, row, :, tile(t)]
        return (h, m, ga, gb)[f - 6][row, :, tile(t)]

    def strip(f, e):
        return jnp.where(lane >= 64, field(f, e, 1), field(f, e, 0))

    total = {}
    for b in range(3):
        rows = [r for r in range(FIRST[b], FIRST[b] + 16) if 0 <= r < ROWS]
        masks = [(lane >= (r - FIRST[b]) * 8) & (lane < (r - FIRST[b]) * 8 + 4) for r in rows]
        for f in range(FIELDS):
            x = jnp.zeros((LEVELS, LANES), F32)
            for r, mask in zip(rows, masks):
                x = jnp.where(mask, turn(strip(f, r + 2), (r - FIRST[b]) * 8 - 126), x)
            total[f, b] = x
    packs = {}
    for b in range(3):
        for s in range(2):
            x = jnp.zeros((LEVELS, LANES), F32)
            for f in range(8 * s, min(8 * s + 8, FIELDS)):
                x = jnp.where(slot == f - 8 * s, turn(total[f, b], f - 8 * s - 1), x)
            packs[0, b, s] = x
        for s in range(3):
            x = jnp.zeros((LEVELS, LANES), F32)
            for f in range(4 * s, min(4 * s + 4, FIELDS)):
                at = 2 * (f - 4 * s)
                x = jnp.where((slot >> 1) == f - 4 * s, turn(total[f, b], at - 2), x)
            packs[1, b, s] = x
    for (n, b, s), x in packs.items():
        (to_right, to_left)[n][b, s] = x
    for (f, b), x in total.items():
        own[f, b] = x

    pl.semaphore_wait(barrier, len(TARGETS))
    pl.semaphore_signal(corner_sem, inc=1, device_id=device(*RIGHT), device_id_type=MESH)

    sends = []

    def send(src, dst, target):
        n = len(sends)
        sends.append(
            pltpu.make_async_remote_copy(
                src_ref=src, dst_ref=dst, send_sem=send_sem.at[n], recv_sem=recv_sem.at[n],
                device_id=device(*target), device_id_type=MESH,
            )
        )
        sends[-1].start()

    top, bottom = pl.ds(0, 2), pl.ds(EXT - 2, 2)
    last, lead = pl.ds(ROWS, 2), pl.ds(2, 2)
    for ref in (v, w):
        send(ref.at[0:2, last], ref.at[0:2, top], DOWN)
        send(ref.at[2, ROWS + 1], ref.at[2, 1], DOWN)
        send(ref.at[1:3, lead], ref.at[1:3, bottom], UP)
        send(ref.at[0, 2], ref.at[0, EXT - 2], UP)
    for ref in (h, m, ga, gb):
        send(ref.at[last], ref.at[top], DOWN)
        send(ref.at[lead], ref.at[bottom], UP)
    send(to_left.at[2], corner_tr, DOWN_LEFT)
    send(to_right.at[0], corner_bl, UP_RIGHT)
    send(to_right, from_left, RIGHT)
    send(to_left, from_right, LEFT)

    def invert(row):
        return [1.0 / ga[row, :, tile(t)] for t in range(2)]

    def keep(row, values):
        for t in range(2):
            inverse[row, :, tile(t)] = values[t]

    staged(range(2, ROWS + 2), invert, keep, 8)
    turned_rows(range(2, ROWS + 2), v, h, w, m, ga, turned)
    pl.semaphore_wait(corner_sem, 1)
    send(to_left.at[0], corner_br, UP_LEFT)
    energy_rows(range(3, ROWS + 1), v, w, ga, gb, inverse, kin)

    def group(index, _):
        base = 3 + index * GROUP
        vertex_rows([(j, base + j) for j in range(GROUP)], v, h, w, m, ga, gb, turned, sums)
        return 0

    lax.fori_loop(0, (ROWS - 2) // GROUP, group, 0)
    cell_rows(range(4, ROWS), sums, cell)

    for copy in sends:
        copy.wait_recv()

    top_rows, bottom_rows = lane < 16, (lane >= 48) & (lane < 64)
    strips = {}
    for b in range(3):
        right = [from_right[b, s] for s in range(3)]
        left = [from_left[b, s] for s in range(2)]
        if b == 0:
            right = [jnp.where(top_rows, turn(corner_tr[s], -32), right[s]) for s in range(3)]
        if b == 2:
            right = [jnp.where(bottom_rows, turn(corner_br[s], 32), right[s]) for s in range(3)]
            left = [jnp.where(bottom_rows, turn(corner_bl[s], 32), left[s]) for s in range(2)]
        for f in range(FIELDS):
            x = own[f, b]
            for r in ((-2, -1) if b == 0 else ((32, 33) if b == 2 else ())):
                q = (r - FIRST[b]) * 8
                x = jnp.where((lane >= q) & (lane < q + 4), turn(strip(f, r + 2), q - 126), x)
            y = turn(right[f // 4], 2 - 2 * (f % 4))
            z = turn(left[f // 8], 4 - f % 8)
            strips[f, b] = jnp.where(slot < 2, x, jnp.where(slot < 4, y, jnp.where(slot == 4, z, turn(x, 3))))
    turned_rows((0, 1, EXT - 2, EXT - 1), v, h, w, m, ga, turned)
    for (f, b), x in strips.items():
        rim[f, b] = x

    results = {}

    def shift(x, di, dj):
        return turn(x, -(8 * di + dj))

    for b in range(3):

        def geo(f, plane):
            return jnp.broadcast_to(rim[f, b, pl.ds(plane, 1), :], (LEVELS, LANES))

        vv, ww = [rim[k, b] for k in range(3)], [rim[3 + k, b] for k in range(3)]
        hh, mm = rim[6, b], rim[7, b]
        d = [geo(8, k) for k in range(3)]
        f = [vv[k] * d[k] for k in range(3)]
        g = [ww[k] * d[k] for k in range(3)]
        h_right, m_right = shift(hh, 0, 1), shift(mm, 0, 1)
        v0, w0 = first_vertex(
            geo(8, 4), geo(9, 0), geo(9, 1), geo(9, 2), f[0], f[1], shift(f[2], 1, 0), g[0], g[1], shift(g[2], 1, 0),
            hh, shift(hh, 1, 0), h_right, mm, shift(mm, 1, 0), m_right,
        )
        v1, w1 = second_vertex(
            geo(8, 5), geo(9, 3), geo(9, 4), geo(9, 5), f[1], f[2], shift(f[0], -1, 1), g[1], g[2], shift(g[0], -1, 1),
            hh, h_right, shift(hh, -1, 1), mm, m_right, shift(mm, -1, 1),
        )
        length = (geo(8, 6), geo(8, 7), geo(9, 6))
        e = [energy_of(vv[k], ww[k], d[k], length[k]) for k in range(3)]
        energy = (e[0] + e[1] + e[2] + shift(e[0], -1, 0) + (shift(e[1], 0, -1) + shift(e[2], 1, -1))) / geo(8, 3)
        results[0, 0, b] = jnp.where(slot == 0, shift(v0, 0, 1), shift(energy, 0, 4))
        results[0, 1, b] = jnp.where(slot == 0, shift(v1, 0, 1), shift(v1, 1, 3))
        for n, (x0, x1) in enumerate(((v0, v1), (w0, w1))):
            here = x0 + x1
            mean = (here + shift(x0, -1, 0) + (shift(here, 0, -1) + shift(x1, 1, -1))) * (1.0 / 6.0)
            results[1, n, b] = jnp.where(slot == 0, shift(mean, 0, 1), shift(mean, 0, 4))
            results[2, n, b] = mean
    for (which, n, b), x in results.items():
        (rim_patch, rim_c, rim_right)[which][n, b] = x

    vertex_rows([(e, e) for e in (0, 1, 2, ROWS + 1, ROWS + 2, ROWS + 3)], v, h, w, m, ga, gb, turned, sums, 2, EXT - 1, 0)
    energy_rows((2, ROWS + 1), v, w, ga, gb, inverse, kin)
    cell_rows((1, 2, 3, ROWS, ROWS + 1, ROWS + 2), sums, cell)
    for copy in sends:
        copy.wait_send()


def output_kernel(
    v, w, sums, cell, kin, inverse, rim_patch, rim_c, rim_right,
    vertex_out, kinetic_out, cell_out, edge_out,
    vertex_buf, kinetic_buf, cell_buf, edge_buf, other_buf, right_buf, corner_buf, sem,
):
    lane = lane_id()
    is_last, is_first, tail = lane == LANES - 1, lane == 0, lane >= LANES - 2

    def pick(ref, n, row, s, to):
        block, q = rim_of(row)
        return turn(ref[n, block], to - (q + s))

    copies = []

    def put(src, dst):
        copies.append(pltpu.make_async_copy(src, dst, sem.at[len(copies)]))
        copies[-1].start()

    def begin(r):
        values = []
        for n in range(2):
            pair = row_pair(cell, n, r + 2)
            values += [pair, turn(pair[0], -1), turn(pair[1], -1), pick(rim_c, n, r, 0, LANES - 1), pick(rim_right, n, r, 1, LANES - 2)]
        if r < ROWS:
            values += [row_pair(sums, 0, r + 2), pick(rim_patch, 0, r, 0, LANES - 1)]
            if r >= 0:
                values += [row_pair(sums, 2, r + 2), row_pair(kin, r), pick(rim_patch, 1, r, 0, LANES - 1)]
                below = row_pair(sums, 2, r + 3)
                values += [turn(below[0], 1), turn(below[1], 1)]
        return values

    def finish(r, values):
        for n, buf in ((0, cell_buf), (1, other_buf)):
            pair, first, second, patch, patch_right = values[5 * n : 5 * n + 5]
            buf[r + 1, :, tile(0)] = jnp.where(is_first, patch, pair[0])
            buf[r + 1, :, tile(1)] = jnp.where(is_last, patch, pair[1])
            right_buf[n, r + 1, :, tile(0)] = jnp.where(is_last, second, first)
            right_buf[n, r + 1, :, tile(1)] = jnp.where(tail, patch_right, second)
        if r < ROWS:
            v0, patch = values[10:12]
            vertex_buf[0, r + 1, :, tile(0)] = v0[0]
            vertex_buf[0, r + 1, :, tile(1)] = jnp.where(is_last, patch, v0[1])
            if r >= 0:
                v1, energy, other, first, second = values[12:17]
                kinetic_buf[r, :, tile(0)] = jnp.where(is_first, patch, energy[0])
                kinetic_buf[r, :, tile(1)] = energy[1]
                vertex_buf[1, r + 1, :, tile(0)] = v1[0]
                vertex_buf[1, r + 1, :, tile(1)] = jnp.where(is_last, other, v1[1])
                corner_buf[r, :, tile(0)] = jnp.where(is_first, other, first)
                corner_buf[r, :, tile(1)] = jnp.where(is_first, first, second)

    staged(range(-1, ROWS + 1), begin, finish, 8)
    for k in range(LEVELS):
        put(vertex_buf.at[:, 1 : ROWS + 1, k], vertex_out.at[:, k])
        put(kinetic_buf.at[:, k], kinetic_out.at[k])
        put(cell_buf.at[1 : ROWS + 1, k], cell_out.at[k])

    def slopes(r):
        v0, v1 = row_pair(vertex_buf, 0, r + 1), row_pair(vertex_buf, 1, r + 1)
        means = (
            both(add, v0, row_pair(corner_buf, r)),
            both(add, v0, v1),
            both(add, v1, row_pair(vertex_buf, 0, r)),
        )
        here = (row_pair(cell_buf, r + 1), row_pair(other_buf, r + 1))
        lower = (row_pair(cell_buf, r + 2), row_pair(other_buf, r + 2))
        right = (row_pair(right_buf, 0, r + 1), row_pair(right_buf, 1, r + 1))
        upper = (row_pair(right_buf, 0, r), row_pair(right_buf, 1, r))
        values = []
        for k, side in enumerate((lower, right, upper)):
            velocity, tendency = row_pair(v, k, r + 2), row_pair(w, k, r + 2)
            factor = spread_pair(inverse, r + 2, k)
            for t in range(2):
                slope = velocity[t] * (side[0][t] - here[0][t]) + tendency[t] * (side[1][t] - here[1][t])
                values.append(0.5 * (means[k][t] - slope * factor[t]))
        return values

    def keep(r, values):
        for k in range(3):
            for t in range(2):
                edge_buf[k, r, :, tile(t)] = values[2 * k + t]

    half = ROWS // 2
    for part in range(2):
        rows = pl.ds(part * half, half)
        staged(range(part * half, (part + 1) * half), slopes, keep, 3)
        for k in range(LEVELS):
            put(edge_buf.at[:, rows, k], edge_out.at[:, k, rows])
    for copy in copies:
        copy.wait()


def local(*args):
    args = [pltpu.with_memory_space_constraint(x, pltpu.HBM) for x in args]
    whole = pl.BlockSpec(memory_space=pltpu.VMEM)
    anywhere = pl.BlockSpec(memory_space=pl.ANY)
    wide = (LEVELS, 2 * LANES)
    thin = (LEVELS, LANES)
    passed = [
        (3, EXT, *wide), (3, EXT, *wide), (4, EXT, *wide), (2, EXT, *wide), (ROWS, *wide), (EXT, *wide),
        (2, 3, *thin), (2, 3, *thin), (2, 3, *thin),
    ]
    grant = 24 << 20
    between = pl.pallas_call(
        exchange_kernel,
        out_shape=[pltpu.VMEM(s, F32) for s in passed],
        in_specs=[anywhere] * 9,
        out_specs=[whole] * len(passed),
        scratch_shapes=[
            pltpu.VMEM((EXT, *wide), F32), pltpu.VMEM((EXT, *wide), F32),
            pltpu.VMEM((EXT, *wide), F32), pltpu.VMEM((EXT, *wide), F32),
            pltpu.VMEM((4, EXT, *wide), F32), pltpu.VMEM((FIELDS, 3, *thin), F32),
            pltpu.VMEM((3, 2, *thin), F32), pltpu.VMEM((3, 3, *thin), F32),
            pltpu.VMEM((3, 2, *thin), F32), pltpu.VMEM((3, 3, *thin), F32),
            pltpu.VMEM((3, *thin), F32), pltpu.VMEM((3, *thin), F32), pltpu.VMEM((2, *thin), F32),
            pltpu.VMEM((FIELDS, 3, *thin), F32),
            pltpu.SemaphoreType.DMA((48,)), pltpu.SemaphoreType.DMA((21,)), pltpu.SemaphoreType.DMA((21,)),
            pltpu.SemaphoreType.REGULAR,
        ],
        compiler_params=pltpu.CompilerParams(collective_id=0, has_side_effects=True, vmem_limit_bytes=grant),
    )(*args)
    outs = [(2, LEVELS, ROWS, 2 * LANES), (LEVELS, ROWS, 2 * LANES), (LEVELS, ROWS, 2 * LANES), (3, LEVELS, ROWS, 2 * LANES)]
    return tuple(
        pl.pallas_call(
            output_kernel,
            out_shape=[jax.ShapeDtypeStruct(s, F32) for s in outs],
            in_specs=[whole] * len(passed),
            out_specs=[anywhere] * 4,
            scratch_shapes=[
                pltpu.VMEM((2, ROWS + 1, *wide), F32), pltpu.VMEM((ROWS, *wide), F32),
                pltpu.VMEM((ROWS + 2, *wide), F32), pltpu.VMEM((3, ROWS, *wide), F32),
                pltpu.VMEM((ROWS + 2, *wide), F32), pltpu.VMEM((2, ROWS + 2, *wide), F32), pltpu.VMEM((ROWS, *wide), F32),
                pltpu.SemaphoreType.DMA((64,)),
            ],
            compiler_params=pltpu.CompilerParams(vmem_limit_bytes=grant),
        )(*between)
    )


def solution(mesh):
    edges, cell = P(None, None, "py", "px"), P(None, "py", "px")
    return jax.shard_map(
        local,
        mesh=mesh,
        in_specs=(edges, cell, edges, cell, cell, cell, P("py", "px"), edges, cell),
        out_specs=(edges, cell, cell, edges),
        check_vma=False,
    )
```

```python
import jax
import jax.numpy as jnp
from jax import lax
from jax.experimental import pallas as pl
from jax.experimental.pallas import tpu as pltpu
from jax.sharding import PartitionSpec as P

F32 = jnp.float32
MESH = pl.DeviceIdType.MESH
ROWS = 32
EXT = ROWS + 4
LEVELS = 8
LANES = 128

FIRST = (-2, 12, 26)
FIELDS = 10
GROUP = 6

DOWN, UP, RIGHT, LEFT = (1, 0), (-1, 0), (0, 1), (0, -1)
DOWN_LEFT, UP_LEFT, UP_RIGHT = (1, -1), (-1, -1), (-1, 1)


def rim_of(row):
    block = 0 if row <= 12 else (1 if row <= 26 else 2)
    return block, (row - FIRST[block]) * 8


def lane_id():
    return lax.broadcasted_iota(jnp.int32, (LEVELS, LANES), 1)


def turn(x, amount):
    amount = amount % LANES
    return x if amount == 0 else pltpu.roll(x, amount, 1)


def next_col(pair, lane):
    first, second = turn(pair[0], -1), turn(pair[1], -1)
    return jnp.where(lane == LANES - 1, second, first), second


def prev_col(pair, lane):
    first, second = turn(pair[0], 1), turn(pair[1], 1)
    return first, jnp.where(lane == 0, first, second)


def tile(t):
    return pl.ds(t * LANES, LANES)


def row_pair(ref, *index):
    return ref[(*index, slice(None), tile(0))], ref[(*index, slice(None), tile(1))]


def spread(ref, row, plane, t):
    return jnp.broadcast_to(ref[row, pl.ds(plane, 1), tile(t)], (LEVELS, LANES))


def spread_pair(ref, row, plane):
    return spread(ref, row, plane, 0), spread(ref, row, plane, 1)


def both(fn, *pairs):
    return tuple(fn(*(p[t] for p in pairs)) for t in range(2))


def add(a, b):
    return a + b


def mul(a, b):
    return a * b


def staged(rows, begin, finish, depth):
    waiting = []
    for row in rows:
        waiting.append((row, begin(row)))
        if len(waiting) > depth:
            finish(*waiting.pop(0))
    for row, value in waiting:
        finish(row, value)


def weigh(n0, n1, s0, s1):
    start = n0 / s0
    middle = (n0 + n0 + n1) / (s0 + s0 + s1)
    end = (n0 + n1) / (s0 + s1)
    twice = middle + middle
    late = twice + end
    return (start + twice + late) * (1.0 / 6.0), late * (1.0 / 6.0)


def first_vertex(cor, k0, k1, k2, f0, f1, f2_down, g0, g1, g2_down, h, h_down, h_right, m, m_down, m_right):
    n0 = cor * (k0 + k1 + k2) + (f0 + f2_down - f1)
    n1 = g0 + g2_down - g1
    s0 = k0 * h + k1 * h_down + k2 * h_right
    s1 = k0 * m + k1 * m_down + k2 * m_right
    return weigh(n0, n1, s0, s1)


def second_vertex(cor, k0, k1, k2, f1, f2, f0_diag, g1, g2, g0_diag, h, h_right, h_diag, m, m_right, m_diag):
    n0 = cor * (k0 + k1 + k2) + (f1 - f2 - f0_diag)
    n1 = g1 - g2 - g0_diag
    s0 = k0 * h + k1 * h_right + k2 * h_diag
    s1 = k0 * m + k1 * m_right + k2 * m_diag
    return weigh(n0, n1, s0, s1)


def energy_of(v, w, d, e):
    return (v * (v + w) + (w * w) * (1.0 / 3.0)) * (0.25 * d * e)


def turned_rows(rows, v, h, w, m, ga, right):
    def begin(row):
        d0 = spread_pair(ga, row, 0)
        pairs = (both(mul, row_pair(v, 0, row), d0), both(mul, row_pair(w, 0, row), d0), row_pair(h, row), row_pair(m, row))
        return [(turn(p[0], -1), turn(p[1], -1)) for p in pairs]

    def finish(row, turned):
        last = lane_id() == LANES - 1
        for n, (first, second) in enumerate(turned):
            right[n, row, :, tile(0)] = jnp.where(last, second, first)
            right[n, row, :, tile(1)] = second

    staged(rows, begin, finish, 8)


def vertex_rows(rows, v, h, w, m, ga, gb, right, out, depth=2, skip_first=None, skip_second=None):
    known = {}

    def flux(ref, name, k, row, key):
        if (name, k, key) not in known:
            known[name, k, key] = both(mul, row_pair(ref, k, row), spread_pair(ga, row, k))
        return known[name, k, key]

    def begin(item):
        key, row = item
        f = [flux(v, "v", k, row, key) for k in range(3)]
        g = [flux(w, "w", k, row, key) for k in range(3)]
        hh, mm = row_pair(h, row), row_pair(m, row)
        h_right, m_right = row_pair(right, 2, row), row_pair(right, 3, row)
        results = []
        if key != skip_first:
            below = row + 1
            f2_down, g2_down = flux(v, "v", 2, below, key + 1), flux(w, "w", 2, below, key + 1)
            h_down, m_down = row_pair(h, below), row_pair(m, below)
            cor = spread_pair(ga, row, 4)
            kite = [spread_pair(gb, row, p) for p in range(3)]
            for t in range(2):
                pair = first_vertex(
                    cor[t], kite[0][t], kite[1][t], kite[2][t], f[0][t], f[1][t], f2_down[t], g[0][t], g[1][t],
                    g2_down[t], hh[t], h_down[t], h_right[t], mm[t], m_down[t], m_right[t],
                )
                results += [(0, t, pair[0]), (1, t, pair[1])]
        if key != skip_second:
            above = row - 1
            f0_diag, g0_diag, h_diag, m_diag = (row_pair(right, n, above) for n in range(4))
            cor = spread_pair(ga, row, 5)
            kite = [spread_pair(gb, row, p) for p in range(3, 6)]
            for t in range(2):
                pair = second_vertex(
                    cor[t], kite[0][t], kite[1][t], kite[2][t], f[1][t], f[2][t], f0_diag[t], g[1][t], g[2][t],
                    g0_diag[t], hh[t], h_right[t], h_diag[t], mm[t], m_right[t], m_diag[t],
                )
                results += [(2, t, pair[0]), (3, t, pair[1])]
        return results

    def finish(item, results):
        for n, t, value in results:
            out[n, item[1], :, tile(t)] = value

    staged(rows, begin, finish, depth)


def cell_rows(rows, sums, out):
    def begin(row):
        values = []
        for n in range(2):
            v0, v1 = row_pair(sums, n, row), row_pair(sums, 2 + n, row)
            above, below = row_pair(sums, n, row - 1), row_pair(sums, 2 + n, row + 1)
            here = both(add, v0, v1)
            west = both(add, here, below)
            values.append((both(add, here, above), (turn(west[0], 1), turn(west[1], 1))))
        return values

    def finish(row, values):
        start = lane_id() == 0
        for n, (near, west) in enumerate(values):
            out[n, row, :, tile(0)] = (near[0] + west[0]) * (1.0 / 6.0)
            out[n, row, :, tile(1)] = (near[1] + jnp.where(start, west[0], west[1])) * (1.0 / 6.0)

    staged(rows, begin, finish, 5)


def energy_rows(rows, v, w, ga, gb, inverse, out):
    spots = ((ga, 6), (ga, 7), (gb, 6))
    known = {}

    def one(k, row):
        if (k, row) not in known:
            ref, plane = spots[k]
            known[k, row] = both(
                energy_of, row_pair(v, k, row), row_pair(w, k, row), spread_pair(ga, row, k), spread_pair(ref, row, plane)
            )
        return known[k, row]

    def begin(row):
        e1 = one(1, row)
        near = both(lambda a, b, c, d: a + b + (c + d), one(0, row), one(0, row - 1), e1, one(2, row))
        west = both(add, e1, one(2, row + 1))
        return near, (turn(west[0], 1), turn(west[1], 1))

    def finish(row, values):
        near, west = values
        start = lane_id() == 0
        area = spread_pair(inverse, row, 3)
        out[row - 2, :, tile(0)] = (near[0] + west[0]) * area[0]
        out[row - 2, :, tile(1)] = (near[1] + jnp.where(start, west[0], west[1])) * area[1]

    staged(rows, begin, finish, 6)


def exchange_kernel(
    v_in, h_in, w_in, m_in, cd_in, el_in, ca_in, ka_in, co_in,
    v, w, sums, cell, kin, inverse, rim_patch, rim_c, rim_right,
    h, m, ga, gb, turned, own, to_right, to_left, from_left, from_right, corner_tr, corner_br, corner_bl, rim,
    load_sem, send_sem, recv_sem, left_sem,
):
    ny, nx = lax.axis_size("py"), lax.axis_size("px")
    my, mx = lax.axis_index("py"), lax.axis_index("px")

    def device(dy, dx):
        return {"py": lax.rem(my + dy + ny, ny), "px": lax.rem(mx + dx + nx, nx)}

    barrier = pltpu.get_barrier_semaphore()

    def tell(sem, target):
        pl.semaphore_signal(sem, inc=1, device_id=device(*target), device_id_type=MESH)

    for target in (DOWN, UP, LEFT, DOWN_LEFT):
        tell(barrier, target)

    loads = []

    def load(src, dst):
        loads.append(pltpu.make_async_copy(src, dst, load_sem.at[len(loads)]))
        loads[-1].start()

    mine = pl.ds(2, ROWS)
    for p in range(3):
        load(cd_in.at[p], ga.at[mine, p])
    load(ca_in, ga.at[mine, 3])
    for p in range(2):
        load(co_in.at[p], ga.at[mine, 4 + p])
        load(el_in.at[p], ga.at[mine, 6 + p])
    for a in range(2):
        for p in range(3):
            load(ka_in.at[a, p], gb.at[mine, 3 * a + p])
    load(el_in.at[2], gb.at[mine, 6])
    load(el_in.at[2], gb.at[mine, 7])
    steps = [len(loads)]
    for src, dst in ((h_in, h), (m_in, m)):
        for k in range(LEVELS):
            load(src.at[k], dst.at[mine, k])
    steps.append(len(loads))
    for src, dst in ((v_in, v), (w_in, w)):
        for k in range(LEVELS):
            load(src.at[:, k], dst.at[:, mine, k])
        steps.append(len(loads))

    def arrived(step):
        for copy in loads[steps[step - 1] if step else 0 : steps[step]]:
            copy.wait()

    lane = lane_id()
    slot = lane & 7

    def field(f, row, t):
        if f < 3:
            return v[f, row, :, tile(t)]
        if f < 6:
            return w[f - 3, row, :, tile(t)]
        return (h, m, ga, gb)[f - 6][row, :, tile(t)]

    def strip(f, e):
        return jnp.where(lane >= 64, field(f, e, 1), field(f, e, 0))

    total = {}
    for step, fields in enumerate(((8, 9), (6, 7), (0, 1, 2), (3, 4, 5))):
        arrived(step)
        for b in (2, 0, 1):
            rows = [r for r in range(FIRST[b], FIRST[b] + 16) if 0 <= r < ROWS]
            masks = [(lane >= (r - FIRST[b]) * 8) & (lane < (r - FIRST[b]) * 8 + 4) for r in rows]
            for f in fields:
                x = jnp.zeros((LEVELS, LANES), F32)
                for r, mask in zip(rows, masks):
                    x = jnp.where(mask, turn(strip(f, r + 2), (r - FIRST[b]) * 8 - 126), x)
                total[f, b] = x
    packs = {}
    for b in (2, 0, 1):
        for s in range(3):
            x = jnp.zeros((LEVELS, LANES), F32)
            for f in range(4 * s, min(4 * s + 4, FIELDS)):
                at = 2 * (f - 4 * s)
                x = jnp.where((slot >> 1) == f - 4 * s, turn(total[f, b], at - 2), x)
            packs[1, b, s] = x
        for s in range(2):
            x = jnp.zeros((LEVELS, LANES), F32)
            for f in range(8 * s, min(8 * s + 8, FIELDS)):
                x = jnp.where(slot == f - 8 * s, turn(total[f, b], f - 8 * s - 1), x)
            packs[0, b, s] = x
    for (n, b, s), x in packs.items():
        (to_right, to_left)[n][b, s] = x
    for (f, b), x in total.items():
        own[f, b] = x

    pl.semaphore_wait(barrier, 4)
    tell(left_sem, RIGHT)

    sends = []

    def send(src, dst, target):
        n = len(sends)
        sends.append(
            pltpu.make_async_remote_copy(
                src_ref=src, dst_ref=dst, send_sem=send_sem.at[n], recv_sem=recv_sem.at[n],
                device_id=device(*target), device_id_type=MESH,
            )
        )
        sends[-1].start()
        return sends[-1]

    top, bottom = pl.ds(0, 2), pl.ds(EXT - 2, 2)
    last, lead = pl.ds(ROWS, 2), pl.ds(2, 2)
    row_sends, rim_sends = [], []
    for ref in (v, w):
        row_sends.append(send(ref.at[0:2, last], ref.at[0:2, top], DOWN))
        row_sends.append(send(ref.at[1:3, lead], ref.at[1:3, bottom], UP))
        row_sends.append(send(ref.at[2, ROWS + 1], ref.at[2, 1], DOWN))
        row_sends.append(send(ref.at[0, 2], ref.at[0, EXT - 2], UP))
    for ref in (h, m, ga, gb):
        row_sends.append(send(ref.at[last], ref.at[top], DOWN))
        row_sends.append(send(ref.at[lead], ref.at[bottom], UP))
    rim_sends.append(send(to_right.at[0], corner_bl, UP_RIGHT))
    rim_sends.append(send(to_right, from_left, RIGHT))

    def invert(row):
        return [1.0 / ga[row, :, tile(t)] for t in range(2)]

    def keep(row, values):
        for t in range(2):
            inverse[row, :, tile(t)] = values[t]

    staged(range(2, ROWS + 2), invert, keep, 8)
    turned_rows(range(2, ROWS + 2), v, h, w, m, ga, turned)
    energy_rows(range(3, ROWS + 1), v, w, ga, gb, inverse, kin)
    pl.semaphore_wait(left_sem, 1)
    rim_sends.append(send(to_left.at[2], corner_tr, DOWN_LEFT))
    rim_sends.append(send(to_left, from_right, LEFT))
    rim_sends.append(send(to_left.at[0], corner_br, UP_LEFT))

    def group(index, _):
        base = 3 + index * GROUP
        vertex_rows([(j, base + j) for j in range(GROUP)], v, h, w, m, ga, gb, turned, sums)
        return 0

    lax.fori_loop(0, (ROWS - 2) // GROUP, group, 0)
    cell_rows(range(4, ROWS), sums, cell)

    for copy in row_sends:
        copy.wait_recv()
    turned_rows((0, 1, EXT - 2, EXT - 1), v, h, w, m, ga, turned)
    vertex_rows([(e, e) for e in (0, 1, 2, ROWS + 1, ROWS + 2, ROWS + 3)], v, h, w, m, ga, gb, turned, sums, 2, EXT - 1, 0)
    energy_rows((2, ROWS + 1), v, w, ga, gb, inverse, kin)
    cell_rows((1, 2, 3, ROWS, ROWS + 1, ROWS + 2), sums, cell)
    merged = {}
    for b in range(3):
        for f in range(FIELDS):
            x = own[f, b]
            for r in ((-2, -1) if b == 0 else ((32, 33) if b == 2 else ())):
                q = (r - FIRST[b]) * 8
                x = jnp.where((lane >= q) & (lane < q + 4), turn(strip(f, r + 2), q - 126), x)
            merged[f, b] = jnp.where(slot < 2, x, turn(x, 3))
    for (f, b), x in merged.items():
        own[f, b] = x

    for copy in rim_sends:
        copy.wait_recv()

    top_rows, bottom_rows = lane < 16, (lane >= 48) & (lane < 64)
    strips = {}
    for b in range(3):
        right = [from_right[b, s] for s in range(3)]
        left = [from_left[b, s] for s in range(2)]
        if b == 0:
            right = [jnp.where(top_rows, turn(corner_tr[s], -32), right[s]) for s in range(3)]
        if b == 2:
            right = [jnp.where(bottom_rows, turn(corner_br[s], 32), right[s]) for s in range(3)]
            left = [jnp.where(bottom_rows, turn(corner_bl[s], 32), left[s]) for s in range(2)]
        for f in range(FIELDS):
            y = turn(right[f // 4], 2 - 2 * (f % 4))
            z = turn(left[f // 8], 4 - f % 8)
            strips[f, b] = jnp.where((slot >> 1) == 1, y, jnp.where(slot == 4, z, own[f, b]))
    for (f, b), x in strips.items():
        rim[f, b] = x

    results = {}

    def shift(x, di, dj):
        return turn(x, -(8 * di + dj))

    for b in range(3):

        def geo(f, plane):
            return jnp.broadcast_to(rim[f, b, pl.ds(plane, 1), :], (LEVELS, LANES))

        vv, ww = [rim[k, b] for k in range(3)], [rim[3 + k, b] for k in range(3)]
        hh, mm = rim[6, b], rim[7, b]
        d = [geo(8, k) for k in range(3)]
        f = [vv[k] * d[k] for k in range(3)]
        g = [ww[k] * d[k] for k in range(3)]
        h_right, m_right = shift(hh, 0, 1), shift(mm, 0, 1)
        v0, w0 = first_vertex(
            geo(8, 4), geo(9, 0), geo(9, 1), geo(9, 2), f[0], f[1], shift(f[2], 1, 0), g[0], g[1], shift(g[2], 1, 0),
            hh, shift(hh, 1, 0), h_right, mm, shift(mm, 1, 0), m_right,
        )
        v1, w1 = second_vertex(
            geo(8, 5), geo(9, 3), geo(9, 4), geo(9, 5), f[1], f[2], shift(f[0], -1, 1), g[1], g[2], shift(g[0], -1, 1),
            hh, h_right, shift(hh, -1, 1), mm, m_right, shift(mm, -1, 1),
        )
        length = (geo(8, 6), geo(8, 7), geo(9, 6))
        e = [energy_of(vv[k], ww[k], d[k], length[k]) for k in range(3)]
        energy = (e[0] + e[1] + e[2] + shift(e[0], -1, 0) + (shift(e[1], 0, -1) + shift(e[2], 1, -1))) / geo(8, 3)
        results[0, 0, b] = jnp.where(slot == 0, shift(v0, 0, 1), shift(energy, 0, 4))
        results[0, 1, b] = jnp.where(slot == 0, shift(v1, 0, 1), shift(v1, 1, 3))
        for n, (x0, x1) in enumerate(((v0, v1), (w0, w1))):
            here = x0 + x1
            mean = (here + shift(x0, -1, 0) + (shift(here, 0, -1) + shift(x1, 1, -1))) * (1.0 / 6.0)
            results[1, n, b] = jnp.where(slot == 0, shift(mean, 0, 1), shift(mean, 0, 4))
            results[2, n, b] = mean
    for (which, n, b), x in results.items():
        (rim_patch, rim_c, rim_right)[which][n, b] = x

    for copy in sends:
        copy.wait_send()


def output_kernel(
    v, w, sums, cell, kin, inverse, rim_patch, rim_c, rim_right,
    vertex_out, kinetic_out, cell_out, edge_out,
    vertex_buf, kinetic_buf, cell_buf, edge_buf, other_buf, right_buf, corner_buf, sem,
):
    lane = lane_id()
    is_last, is_first, tail = lane == LANES - 1, lane == 0, lane >= LANES - 2

    def pick(ref, n, row, s, to):
        block, q = rim_of(row)
        return turn(ref[n, block], to - (q + s))

    copies = []

    def put(src, dst):
        copies.append(pltpu.make_async_copy(src, dst, sem.at[len(copies)]))
        copies[-1].start()

    def begin_patch(r):
        values = [row_pair(sums, 0, r + 2), pick(rim_patch, 0, r, 0, LANES - 1)]
        if r >= 0:
            values += [row_pair(sums, 2, r + 2), row_pair(kin, r), pick(rim_patch, 1, r, 0, LANES - 1)]
        return values

    def finish_patch(r, values):
        v0, patch = values[0:2]
        vertex_buf[0, r + 1, :, tile(0)] = v0[0]
        vertex_buf[0, r + 1, :, tile(1)] = jnp.where(is_last, patch, v0[1])
        if r >= 0:
            v1, energy, other = values[2:5]
            kinetic_buf[r, :, tile(0)] = jnp.where(is_first, patch, energy[0])
            kinetic_buf[r, :, tile(1)] = energy[1]
            vertex_buf[1, r + 1, :, tile(0)] = v1[0]
            vertex_buf[1, r + 1, :, tile(1)] = jnp.where(is_last, other, v1[1])
            corner_buf[r, :, tile(0)] = other

    staged(range(-1, ROWS), begin_patch, finish_patch, 8)
    for k in range(LEVELS):
        put(vertex_buf.at[:, 1 : ROWS + 1, k], vertex_out.at[:, k])
        put(kinetic_buf.at[:, k], kinetic_out.at[k])

    def begin_cell(r):
        values = []
        for n in range(2):
            pair = row_pair(cell, n, r + 2)
            values += [pair, turn(pair[0], -1), turn(pair[1], -1), pick(rim_c, n, r, 0, LANES - 1), pick(rim_right, n, r, 1, LANES - 2)]
        return values

    def finish_cell(r, values):
        for n, buf in ((0, cell_buf), (1, other_buf)):
            pair, first, second, patch, patch_right = values[5 * n : 5 * n + 5]
            buf[r + 1, :, tile(0)] = jnp.where(is_first, patch, pair[0])
            buf[r + 1, :, tile(1)] = jnp.where(is_last, patch, pair[1])
            right_buf[n, r + 1, :, tile(0)] = jnp.where(is_last, second, first)
            right_buf[n, r + 1, :, tile(1)] = jnp.where(tail, patch_right, second)

    staged(range(-1, ROWS + 1), begin_cell, finish_cell, 8)
    for k in range(LEVELS):
        put(cell_buf.at[1 : ROWS + 1, k], cell_out.at[k])

    def begin_corner(r):
        below = row_pair(sums, 2, r + 3)
        return turn(below[0], 1), turn(below[1], 1), corner_buf[r, :, tile(0)]

    def finish_corner(r, values):
        first, second, other = values
        corner_buf[r, :, tile(0)] = jnp.where(is_first, other, first)
        corner_buf[r, :, tile(1)] = jnp.where(is_first, first, second)

    staged(range(ROWS), begin_corner, finish_corner, 8)

    def slopes(r):
        v0, v1 = row_pair(vertex_buf, 0, r + 1), row_pair(vertex_buf, 1, r + 1)
        means = (
            both(add, v0, row_pair(corner_buf, r)),
            both(add, v0, v1),
            both(add, v1, row_pair(vertex_buf, 0, r)),
        )
        here = (row_pair(cell_buf, r + 1), row_pair(other_buf, r + 1))
        lower = (row_pair(cell_buf, r + 2), row_pair(other_buf, r + 2))
        right = (row_pair(right_buf, 0, r + 1), row_pair(right_buf, 1, r + 1))
        upper = (row_pair(right_buf, 0, r), row_pair(right_buf, 1, r))
        values = []
        for k, side in enumerate((lower, right, upper)):
            velocity, tendency = row_pair(v, k, r + 2), row_pair(w, k, r + 2)
            factor = spread_pair(inverse, r + 2, k)
            for t in range(2):
                slope = velocity[t] * (side[0][t] - here[0][t]) + tendency[t] * (side[1][t] - here[1][t])
                values.append(0.5 * (means[k][t] - slope * factor[t]))
        return values

    def keep(r, values):
        for k in range(3):
            for t in range(2):
                edge_buf[k, r, :, tile(t)] = values[2 * k + t]

    parts = 2
    size = ROWS // parts
    for part in range(parts):
        rows = pl.ds(part * size, size)
        staged(range(part * size, (part + 1) * size), slopes, keep, 3)
        for k in range(LEVELS):
            put(edge_buf.at[:, rows, k], edge_out.at[:, k, rows])
    for copy in copies:
        copy.wait()


def local(*args):
    args = [pltpu.with_memory_space_constraint(x, pltpu.HBM) for x in args]
    whole = pl.BlockSpec(memory_space=pltpu.VMEM)
    anywhere = pl.BlockSpec(memory_space=pl.ANY)
    wide = (LEVELS, 2 * LANES)
    thin = (LEVELS, LANES)
    passed = [
        (3, EXT, *wide), (3, EXT, *wide), (4, EXT, *wide), (2, EXT, *wide), (ROWS, *wide), (EXT, *wide),
        (2, 3, *thin), (2, 3, *thin), (2, 3, *thin),
    ]
    grant = 24 << 20
    between = pl.pallas_call(
        exchange_kernel,
        out_shape=[pltpu.VMEM(s, F32) for s in passed],
        in_specs=[anywhere] * 9,
        out_specs=[whole] * len(passed),
        scratch_shapes=[
            pltpu.VMEM((EXT, *wide), F32), pltpu.VMEM((EXT, *wide), F32),
            pltpu.VMEM((EXT, *wide), F32), pltpu.VMEM((EXT, *wide), F32),
            pltpu.VMEM((4, EXT, *wide), F32), pltpu.VMEM((FIELDS, 3, *thin), F32),
            pltpu.VMEM((3, 2, *thin), F32), pltpu.VMEM((3, 3, *thin), F32),
            pltpu.VMEM((3, 2, *thin), F32), pltpu.VMEM((3, 3, *thin), F32),
            pltpu.VMEM((3, *thin), F32), pltpu.VMEM((3, *thin), F32), pltpu.VMEM((2, *thin), F32),
            pltpu.VMEM((FIELDS, 3, *thin), F32),
            pltpu.SemaphoreType.DMA((48,)), pltpu.SemaphoreType.DMA((21,)), pltpu.SemaphoreType.DMA((21,)),
            pltpu.SemaphoreType.REGULAR,
        ],
        compiler_params=pltpu.CompilerParams(collective_id=0, has_side_effects=True, vmem_limit_bytes=grant),
    )(*args)
    outs = [(2, LEVELS, ROWS, 2 * LANES), (LEVELS, ROWS, 2 * LANES), (LEVELS, ROWS, 2 * LANES), (3, LEVELS, ROWS, 2 * LANES)]
    return tuple(
        pl.pallas_call(
            output_kernel,
            out_shape=[jax.ShapeDtypeStruct(s, F32) for s in outs],
            in_specs=[whole] * len(passed),
            out_specs=[anywhere] * 4,
            scratch_shapes=[
                pltpu.VMEM((2, ROWS + 1, *wide), F32), pltpu.VMEM((ROWS, *wide), F32),
                pltpu.VMEM((ROWS + 2, *wide), F32), pltpu.VMEM((3, ROWS, *wide), F32),
                pltpu.VMEM((ROWS + 2, *wide), F32), pltpu.VMEM((2, ROWS + 2, *wide), F32), pltpu.VMEM((ROWS, *wide), F32),
                pltpu.SemaphoreType.DMA((40,)),
            ],
            compiler_params=pltpu.CompilerParams(vmem_limit_bytes=grant),
        )(*between)
    )


def solution(mesh):
    edges, cell = P(None, None, "py", "px"), P(None, "py", "px")
    return jax.shard_map(
        local,
        mesh=mesh,
        in_specs=(edges, cell, edges, cell, cell, cell, P("py", "px"), edges, cell),
        out_specs=(edges, cell, cell, edges),
        check_vma=False,
    )
```

```python
import jax
import jax.numpy as jnp
from jax import lax
from jax.experimental import pallas as pl
from jax.experimental.pallas import tpu as pltpu
from jax.sharding import PartitionSpec as P

F32 = jnp.float32
MESH = pl.DeviceIdType.MESH
ROWS = 32
EXT = ROWS + 4
LEVELS = 8
LANES = 128

FIRST = (-2, 12, 26)
FIELDS = 10
GROUP = 6

DOWN, UP, RIGHT, LEFT = (1, 0), (-1, 0), (0, 1), (0, -1)
DOWN_LEFT, UP_LEFT, UP_RIGHT = (1, -1), (-1, -1), (-1, 1)


def rim_of(row):
    block = 0 if row <= 12 else (1 if row <= 26 else 2)
    return block, (row - FIRST[block]) * 8


def lane_id():
    return lax.broadcasted_iota(jnp.int32, (LEVELS, LANES), 1)


def turn(x, amount):
    amount = amount % LANES
    return x if amount == 0 else pltpu.roll(x, amount, 1)


def next_col(pair, lane):
    first, second = turn(pair[0], -1), turn(pair[1], -1)
    return jnp.where(lane == LANES - 1, second, first), second


def prev_col(pair, lane):
    first, second = turn(pair[0], 1), turn(pair[1], 1)
    return first, jnp.where(lane == 0, first, second)


def tile(t):
    return pl.ds(t * LANES, LANES)


def row_pair(ref, *index):
    return ref[(*index, slice(None), tile(0))], ref[(*index, slice(None), tile(1))]


def spread(ref, row, plane, t):
    return jnp.broadcast_to(ref[row, pl.ds(plane, 1), tile(t)], (LEVELS, LANES))


def spread_pair(ref, row, plane):
    return spread(ref, row, plane, 0), spread(ref, row, plane, 1)


def both(fn, *pairs):
    return tuple(fn(*(p[t] for p in pairs)) for t in range(2))


def add(a, b):
    return a + b


def mul(a, b):
    return a * b


def staged(rows, begin, finish, depth):
    waiting = []
    for row in rows:
        waiting.append((row, begin(row)))
        if len(waiting) > depth:
            finish(*waiting.pop(0))
    for row, value in waiting:
        finish(row, value)


def weigh(n0, n1, s0, s1):
    start = n0 / s0
    middle = (n0 + n0 + n1) / (s0 + s0 + s1)
    end = (n0 + n1) / (s0 + s1)
    twice = middle + middle
    late = twice + end
    return (start + twice + late) * (1.0 / 6.0), late * (1.0 / 6.0)


def first_vertex(cor, k0, k1, k2, f0, f1, f2_down, g0, g1, g2_down, h, h_down, h_right, m, m_down, m_right):
    n0 = cor * (k0 + k1 + k2) + (f0 + f2_down - f1)
    n1 = g0 + g2_down - g1
    s0 = k0 * h + k1 * h_down + k2 * h_right
    s1 = k0 * m + k1 * m_down + k2 * m_right
    return weigh(n0, n1, s0, s1)


def second_vertex(cor, k0, k1, k2, f1, f2, f0_diag, g1, g2, g0_diag, h, h_right, h_diag, m, m_right, m_diag):
    n0 = cor * (k0 + k1 + k2) + (f1 - f2 - f0_diag)
    n1 = g1 - g2 - g0_diag
    s0 = k0 * h + k1 * h_right + k2 * h_diag
    s1 = k0 * m + k1 * m_right + k2 * m_diag
    return weigh(n0, n1, s0, s1)


def energy_of(v, w, d, e):
    return (v * (v + w) + (w * w) * (1.0 / 3.0)) * (0.25 * d * e)


def turned_rows(rows, v, h, w, m, ga, right):
    def begin(row):
        d0 = spread_pair(ga, row, 0)
        pairs = (both(mul, row_pair(v, 0, row), d0), both(mul, row_pair(w, 0, row), d0), row_pair(h, row), row_pair(m, row))
        return [(turn(p[0], -1), turn(p[1], -1)) for p in pairs]

    def finish(row, turned):
        last = lane_id() == LANES - 1
        for n, (first, second) in enumerate(turned):
            right[n, row, :, tile(0)] = jnp.where(last, second, first)
            right[n, row, :, tile(1)] = second

    staged(rows, begin, finish, 8)


def vertex_rows(rows, v, h, w, m, ga, gb, right, out, depth=2, skip_first=None, skip_second=None):
    known = {}

    def flux(ref, name, k, row, key):
        if (name, k, key) not in known:
            known[name, k, key] = both(mul, row_pair(ref, k, row), spread_pair(ga, row, k))
        return known[name, k, key]

    def begin(item):
        key, row = item
        f = [flux(v, "v", k, row, key) for k in range(3)]
        g = [flux(w, "w", k, row, key) for k in range(3)]
        hh, mm = row_pair(h, row), row_pair(m, row)
        h_right, m_right = row_pair(right, 2, row), row_pair(right, 3, row)
        results = []
        if key != skip_first:
            below = row + 1
            f2_down, g2_down = flux(v, "v", 2, below, key + 1), flux(w, "w", 2, below, key + 1)
            h_down, m_down = row_pair(h, below), row_pair(m, below)
            cor = spread_pair(ga, row, 4)
            kite = [spread_pair(gb, row, p) for p in range(3)]
            for t in range(2):
                pair = first_vertex(
                    cor[t], kite[0][t], kite[1][t], kite[2][t], f[0][t], f[1][t], f2_down[t], g[0][t], g[1][t],
                    g2_down[t], hh[t], h_down[t], h_right[t], mm[t], m_down[t], m_right[t],
                )
                results += [(0, t, pair[0]), (1, t, pair[1])]
        if key != skip_second:
            above = row - 1
            f0_diag, g0_diag, h_diag, m_diag = (row_pair(right, n, above) for n in range(4))
            cor = spread_pair(ga, row, 5)
            kite = [spread_pair(gb, row, p) for p in range(3, 6)]
            for t in range(2):
                pair = second_vertex(
                    cor[t], kite[0][t], kite[1][t], kite[2][t], f[1][t], f[2][t], f0_diag[t], g[1][t], g[2][t],
                    g0_diag[t], hh[t], h_right[t], h_diag[t], mm[t], m_right[t], m_diag[t],
                )
                results += [(2, t, pair[0]), (3, t, pair[1])]
        return results

    def finish(item, results):
        for n, t, value in results:
            out[n, item[1], :, tile(t)] = value

    staged(rows, begin, finish, depth)


def cell_rows(rows, sums, out):
    def begin(row):
        values = []
        for n in range(2):
            v0, v1 = row_pair(sums, n, row), row_pair(sums, 2 + n, row)
            above, below = row_pair(sums, n, row - 1), row_pair(sums, 2 + n, row + 1)
            here = both(add, v0, v1)
            west = both(add, here, below)
            values.append((both(add, here, above), (turn(west[0], 1), turn(west[1], 1))))
        return values

    def finish(row, values):
        start = lane_id() == 0
        for n, (near, west) in enumerate(values):
            out[n, row, :, tile(0)] = (near[0] + west[0]) * (1.0 / 6.0)
            out[n, row, :, tile(1)] = (near[1] + jnp.where(start, west[0], west[1])) * (1.0 / 6.0)

    staged(rows, begin, finish, 5)


def side_rows(cell_at, vertex_at, cell, sums, right, corner):
    def begin(item):
        ref, row, back = item
        pair = row_pair(*ref, row)
        amount = 1 if back else -1
        return turn(pair[0], amount), turn(pair[1], amount)

    def finish(item, values):
        (_, n), row, back = item
        lane = lane_id()
        if back:
            corner[row - 3, :, tile(0)] = values[0]
            corner[row - 3, :, tile(1)] = jnp.where(lane == 0, values[0], values[1])
        else:
            right[n, row - 1, :, tile(0)] = jnp.where(lane == LANES - 1, values[1], values[0])
            right[n, row - 1, :, tile(1)] = values[1]

    items = [((sums, 2), row, True) for row in vertex_at]
    items += [((cell, n), row, False) for row in cell_at for n in range(2)]
    staged(items, begin, finish, 12)


def energy_rows(rows, v, w, ga, gb, inverse, out):
    spots = ((ga, 6), (ga, 7), (gb, 6))
    known = {}

    def one(k, row):
        if (k, row) not in known:
            ref, plane = spots[k]
            known[k, row] = both(
                energy_of, row_pair(v, k, row), row_pair(w, k, row), spread_pair(ga, row, k), spread_pair(ref, row, plane)
            )
        return known[k, row]

    def begin(row):
        e1 = one(1, row)
        near = both(lambda a, b, c, d: a + b + (c + d), one(0, row), one(0, row - 1), e1, one(2, row))
        west = both(add, e1, one(2, row + 1))
        return near, (turn(west[0], 1), turn(west[1], 1))

    def finish(row, values):
        near, west = values
        start = lane_id() == 0
        area = spread_pair(inverse, row, 3)
        out[row - 2, :, tile(0)] = (near[0] + west[0]) * area[0]
        out[row - 2, :, tile(1)] = (near[1] + jnp.where(start, west[0], west[1])) * area[1]

    staged(rows, begin, finish, 6)


def exchange_kernel(
    v_in, h_in, w_in, m_in, cd_in, el_in, ca_in, ka_in, co_in,
    v, w, sums, cell, kin, inverse, side, corner, rim_patch, rim_c, rim_right,
    h, m, ga, gb, turned, own, to_right, to_left, from_left, from_right, corner_tr, corner_br, corner_bl, rim,
    load_sem, send_sem, recv_sem, left_sem,
):
    ny, nx = lax.axis_size("py"), lax.axis_size("px")
    my, mx = lax.axis_index("py"), lax.axis_index("px")

    def device(dy, dx):
        return {"py": lax.rem(my + dy + ny, ny), "px": lax.rem(mx + dx + nx, nx)}

    barrier = pltpu.get_barrier_semaphore()

    def tell(sem, target):
        pl.semaphore_signal(sem, inc=1, device_id=device(*target), device_id_type=MESH)

    for target in (DOWN, UP, LEFT, DOWN_LEFT):
        tell(barrier, target)

    loads = []

    def load(src, dst):
        loads.append(pltpu.make_async_copy(src, dst, load_sem.at[len(loads)]))
        loads[-1].start()

    mine = pl.ds(2, ROWS)
    for p in range(3):
        load(cd_in.at[p], ga.at[mine, p])
    load(ca_in, ga.at[mine, 3])
    for p in range(2):
        load(co_in.at[p], ga.at[mine, 4 + p])
        load(el_in.at[p], ga.at[mine, 6 + p])
    for a in range(2):
        for p in range(3):
            load(ka_in.at[a, p], gb.at[mine, 3 * a + p])
    load(el_in.at[2], gb.at[mine, 6])
    load(el_in.at[2], gb.at[mine, 7])
    steps = [len(loads)]
    for src, dst in ((h_in, h), (m_in, m)):
        for k in range(LEVELS):
            load(src.at[k], dst.at[mine, k])
    steps.append(len(loads))
    for src, dst in ((v_in, v), (w_in, w)):
        for k in range(LEVELS):
            load(src.at[:, k], dst.at[:, mine, k])
        steps.append(len(loads))

    def arrived(step):
        for copy in loads[steps[step - 1] if step else 0 : steps[step]]:
            copy.wait()

    lane = lane_id()
    slot = lane & 7

    def field(f, row, t):
        if f < 3:
            return v[f, row, :, tile(t)]
        if f < 6:
            return w[f - 3, row, :, tile(t)]
        return (h, m, ga, gb)[f - 6][row, :, tile(t)]

    def strip(f, e):
        return jnp.where(lane >= 64, field(f, e, 1), field(f, e, 0))

    total = {}

    def gather(fields):
        for b in (2, 0, 1):
            rows = [r for r in range(FIRST[b], FIRST[b] + 16) if 0 <= r < ROWS]
            masks = [(lane >= (r - FIRST[b]) * 8) & (lane < (r - FIRST[b]) * 8 + 4) for r in rows]
            for f in fields:
                x = jnp.zeros((LEVELS, LANES), F32)
                for r, mask in zip(rows, masks):
                    x = jnp.where(mask, turn(strip(f, r + 2), (r - FIRST[b]) * 8 - 126), x)
                total[f, b] = x

    arrived(0)
    gather((8, 9))
    arrived(1)
    gather((6, 7))
    arrived(2)
    arrived(3)

    pl.semaphore_wait(barrier, 4)
    tell(left_sem, RIGHT)

    sends = []

    def send(src, dst, target):
        n = len(sends)
        sends.append(
            pltpu.make_async_remote_copy(
                src_ref=src, dst_ref=dst, send_sem=send_sem.at[n], recv_sem=recv_sem.at[n],
                device_id=device(*target), device_id_type=MESH,
            )
        )
        sends[-1].start()
        return sends[-1]

    top, bottom = pl.ds(0, 2), pl.ds(EXT - 2, 2)
    last, lead = pl.ds(ROWS, 2), pl.ds(2, 2)
    row_sends, rim_sends = [], []
    for ref in (v, w):
        row_sends.append(send(ref.at[0:2, last], ref.at[0:2, top], DOWN))
        row_sends.append(send(ref.at[1:3, lead], ref.at[1:3, bottom], UP))
        row_sends.append(send(ref.at[2, ROWS + 1], ref.at[2, 1], DOWN))
        row_sends.append(send(ref.at[0, 2], ref.at[0, EXT - 2], UP))
    for ref in (h, m, ga, gb):
        row_sends.append(send(ref.at[last], ref.at[top], DOWN))
        row_sends.append(send(ref.at[lead], ref.at[bottom], UP))
    gather((0, 1, 2))
    gather((3, 4, 5))
    packs = {}
    for b in (2, 0, 1):
        for s in range(3):
            x = jnp.zeros((LEVELS, LANES), F32)
            for f in range(4 * s, min(4 * s + 4, FIELDS)):
                at = 2 * (f - 4 * s)
                x = jnp.where((slot >> 1) == f - 4 * s, turn(total[f, b], at - 2), x)
            packs[1, b, s] = x
        for s in range(2):
            x = jnp.zeros((LEVELS, LANES), F32)
            for f in range(8 * s, min(8 * s + 8, FIELDS)):
                x = jnp.where(slot == f - 8 * s, turn(total[f, b], f - 8 * s - 1), x)
            packs[0, b, s] = x
    for (n, b, s), x in packs.items():
        (to_right, to_left)[n][b, s] = x
    for (f, b), x in total.items():
        own[f, b] = x

    def invert(row):
        return [1.0 / ga[row, :, tile(t)] for t in range(2)]

    def keep(row, values):
        for t in range(2):
            inverse[row, :, tile(t)] = values[t]

    staged(range(2, ROWS + 2), invert, keep, 8)
    rim_sends.append(send(to_right.at[0], corner_bl, UP_RIGHT))
    rim_sends.append(send(to_right, from_left, RIGHT))

    turned_rows(range(2, ROWS + 2), v, h, w, m, ga, turned)
    energy_rows(range(3, ROWS + 1), v, w, ga, gb, inverse, kin)
    pl.semaphore_wait(left_sem, 1)
    rim_sends.append(send(to_left.at[2], corner_tr, DOWN_LEFT))
    rim_sends.append(send(to_left, from_right, LEFT))
    rim_sends.append(send(to_left.at[0], corner_br, UP_LEFT))

    def group(index, _):
        base = 3 + index * GROUP
        vertex_rows([(j, base + j) for j in range(GROUP)], v, h, w, m, ga, gb, turned, sums)
        return 0

    lax.fori_loop(0, (ROWS - 2) // GROUP, group, 0)
    cell_rows(range(4, ROWS), sums, cell)
    side_rows(range(4, ROWS), range(3, ROWS + 1), cell, sums, side, corner)

    for copy in row_sends:
        copy.wait_recv()
    turned_rows((0, 1, EXT - 2, EXT - 1), v, h, w, m, ga, turned)
    vertex_rows([(e, e) for e in (0, 1, 2, ROWS + 1, ROWS + 2, ROWS + 3)], v, h, w, m, ga, gb, turned, sums, 2, EXT - 1, 0)
    energy_rows((2, ROWS + 1), v, w, ga, gb, inverse, kin)
    cell_rows((1, 2, 3, ROWS, ROWS + 1, ROWS + 2), sums, cell)
    side_rows((1, 2, 3, ROWS, ROWS + 1), (ROWS + 1, ROWS + 2), cell, sums, side, corner)
    merged = {}
    for b in range(3):
        for f in range(FIELDS):
            x = own[f, b]
            for r in ((-2, -1) if b == 0 else ((32, 33) if b == 2 else ())):
                q = (r - FIRST[b]) * 8
                x = jnp.where((lane >= q) & (lane < q + 4), turn(strip(f, r + 2), q - 126), x)
            merged[f, b] = jnp.where(slot < 2, x, turn(x, 3))
    for (f, b), x in merged.items():
        own[f, b] = x

    for copy in rim_sends:
        copy.wait_recv()

    top_rows, bottom_rows = lane < 16, (lane >= 48) & (lane < 64)
    strips = {}
    for b in range(3):
        right = [from_right[b, s] for s in range(3)]
        left = [from_left[b, s] for s in range(2)]
        if b == 0:
            right = [jnp.where(top_rows, turn(corner_tr[s], -32), right[s]) for s in range(3)]
        if b == 2:
            right = [jnp.where(bottom_rows, turn(corner_br[s], 32), right[s]) for s in range(3)]
            left = [jnp.where(bottom_rows, turn(corner_bl[s], 32), left[s]) for s in range(2)]
        for f in range(FIELDS):
            y = turn(right[f // 4], 2 - 2 * (f % 4))
            z = turn(left[f // 8], 4 - f % 8)
            strips[f, b] = jnp.where((slot >> 1) == 1, y, jnp.where(slot == 4, z, own[f, b]))
    for (f, b), x in strips.items():
        rim[f, b] = x

    results = {}

    def shift(x, di, dj):
        return turn(x, -(8 * di + dj))

    for b in range(3):

        def geo(f, plane):
            return jnp.broadcast_to(rim[f, b, pl.ds(plane, 1), :], (LEVELS, LANES))

        vv, ww = [rim[k, b] for k in range(3)], [rim[3 + k, b] for k in range(3)]
        hh, mm = rim[6, b], rim[7, b]
        d = [geo(8, k) for k in range(3)]
        f = [vv[k] * d[k] for k in range(3)]
        g = [ww[k] * d[k] for k in range(3)]
        h_right, m_right = shift(hh, 0, 1), shift(mm, 0, 1)
        v0, w0 = first_vertex(
            geo(8, 4), geo(9, 0), geo(9, 1), geo(9, 2), f[0], f[1], shift(f[2], 1, 0), g[0], g[1], shift(g[2], 1, 0),
            hh, shift(hh, 1, 0), h_right, mm, shift(mm, 1, 0), m_right,
        )
        v1, w1 = second_vertex(
            geo(8, 5), geo(9, 3), geo(9, 4), geo(9, 5), f[1], f[2], shift(f[0], -1, 1), g[1], g[2], shift(g[0], -1, 1),
            hh, h_right, shift(hh, -1, 1), mm, m_right, shift(mm, -1, 1),
        )
        length = (geo(8, 6), geo(8, 7), geo(9, 6))
        e = [energy_of(vv[k], ww[k], d[k], length[k]) for k in range(3)]
        energy = (e[0] + e[1] + e[2] + shift(e[0], -1, 0) + (shift(e[1], 0, -1) + shift(e[2], 1, -1))) / geo(8, 3)
        results[0, 0, b] = jnp.where(slot == 0, shift(v0, 0, 1), shift(energy, 0, 4))
        results[0, 1, b] = jnp.where(slot == 0, shift(v1, 0, 1), shift(v1, 1, 3))
        for n, (x0, x1) in enumerate(((v0, v1), (w0, w1))):
            here = x0 + x1
            mean = (here + shift(x0, -1, 0) + (shift(here, 0, -1) + shift(x1, 1, -1))) * (1.0 / 6.0)
            results[1, n, b] = jnp.where(slot == 0, shift(mean, 0, 1), shift(mean, 0, 4))
            results[2, n, b] = mean
    for (which, n, b), x in results.items():
        (rim_patch, rim_c, rim_right)[which][n, b] = x

    for copy in sends:
        copy.wait_send()


def output_kernel(
    v, w, sums, cell, kin, inverse, side, corner, rim_patch, rim_c, rim_right,
    vertex_out, kinetic_out, cell_out, edge_out,
    vertex_buf, kinetic_buf, cell_buf, edge_buf, corner_buf, sem,
):
    lane = lane_id()
    is_last, is_first, tail = lane == LANES - 1, lane == 0, lane >= LANES - 2

    def pick(ref, n, row, s, to):
        block, q = rim_of(row)
        return turn(ref[n, block], to - (q + s))

    copies = []

    def put(src, dst):
        copies.append(pltpu.make_async_copy(src, dst, sem.at[len(copies)]))
        copies[-1].start()

    def begin_patch(r):
        values = [row_pair(sums, 0, r + 2), pick(rim_patch, 0, r, 0, LANES - 1)]
        if r >= 0:
            values += [row_pair(sums, 2, r + 2), row_pair(kin, r), pick(rim_patch, 1, r, 0, LANES - 1)]
        return values

    def finish_patch(r, values):
        v0, patch = values[0:2]
        vertex_buf[0, r + 1, :, tile(0)] = v0[0]
        vertex_buf[0, r + 1, :, tile(1)] = jnp.where(is_last, patch, v0[1])
        if r >= 0:
            v1, energy, other = values[2:5]
            kinetic_buf[r, :, tile(0)] = jnp.where(is_first, patch, energy[0])
            kinetic_buf[r, :, tile(1)] = energy[1]
            vertex_buf[1, r + 1, :, tile(0)] = v1[0]
            vertex_buf[1, r + 1, :, tile(1)] = jnp.where(is_last, other, v1[1])
            corner_buf[r] = other

    staged(range(-1, ROWS), begin_patch, finish_patch, 8)
    for k in range(LEVELS):
        put(vertex_buf.at[:, 1 : ROWS + 1, k], vertex_out.at[:, k])
        put(kinetic_buf.at[:, k], kinetic_out.at[k])

    def begin(r):
        picks = [(pick(rim_c, n, r, 0, LANES - 1), pick(rim_right, n, r, 1, LANES - 2)) for n in range(2)]
        return picks

    cells, sides = {}, {}

    def work(r, picks):
        stores = []
        cells[r] = []
        sides[r] = []
        for n, (patch, patch_side) in enumerate(picks):
            pair = row_pair(cell, n, r + 2)
            cells[r].append((jnp.where(is_first, patch, pair[0]), jnp.where(is_last, patch, pair[1])))
            if r < ROWS:
                pair = row_pair(side, n, r + 1)
                sides[r].append((pair[0], jnp.where(tail, patch_side, pair[1])))
        if 0 <= r < ROWS:
            stores += [(cell_buf, (r,), t, cells[r][0][t]) for t in range(2)]
        q = r - 1
        if q >= 0:
            v0, v1, above = row_pair(vertex_buf, 0, q + 1), row_pair(vertex_buf, 1, q + 1), row_pair(vertex_buf, 0, q)
            back = row_pair(corner, q)
            means = (both(add, v0, (jnp.where(is_first, corner_buf[q], back[0]), back[1])), both(add, v0, v1), both(add, v1, above))
            here = cells[q]
            for k, other in enumerate((cells[r], sides[q], sides[q - 1])):
                velocity, tendency = row_pair(v, k, q + 2), row_pair(w, k, q + 2)
                factor = spread_pair(inverse, q + 2, k)
                for t in range(2):
                    slope = velocity[t] * (other[0][t] - here[0][t]) + tendency[t] * (other[1][t] - here[1][t])
                    stores.append((edge_buf, (k, q), t, 0.5 * (means[k][t] - slope * factor[t])))
        return stores

    def keep(stores):
        for ref, index, t, value in stores:
            ref[(*index, slice(None), tile(t))] = value

    half = ROWS // 2
    rows = list(range(-1, ROWS + 1))
    ahead = {r: begin(r) for r in rows[:8]}
    behind = []
    for r in rows:
        if r + 8 <= ROWS:
            ahead[r + 8] = begin(r + 8)
        behind.append(work(r, ahead.pop(r)))
        if len(behind) > 2:
            keep(behind.pop(0))
        if r in (half, ROWS):
            while behind:
                keep(behind.pop(0))
            part = pl.ds(r - half, half)
            for k in range(LEVELS):
                put(edge_buf.at[:, part, k], edge_out.at[:, k, part])
            for k in range(LEVELS):
                put(cell_buf.at[part, k], cell_out.at[k, part])
    for copy in copies:
        copy.wait()


def local(*args):
    args = [pltpu.with_memory_space_constraint(x, pltpu.HBM) for x in args]
    whole = pl.BlockSpec(memory_space=pltpu.VMEM)
    anywhere = pl.BlockSpec(memory_space=pl.ANY)
    wide = (LEVELS, 2 * LANES)
    thin = (LEVELS, LANES)
    passed = [
        (3, EXT, *wide), (3, EXT, *wide), (4, EXT, *wide), (2, EXT, *wide), (ROWS, *wide), (EXT, *wide),
        (2, ROWS + 1, *wide), (ROWS, *wide),
        (2, 3, *thin), (2, 3, *thin), (2, 3, *thin),
    ]
    grant = 24 << 20
    between = pl.pallas_call(
        exchange_kernel,
        out_shape=[pltpu.VMEM(s, F32) for s in passed],
        in_specs=[anywhere] * 9,
        out_specs=[whole] * len(passed),
        scratch_shapes=[
            pltpu.VMEM((EXT, *wide), F32), pltpu.VMEM((EXT, *wide), F32),
            pltpu.VMEM((EXT, *wide), F32), pltpu.VMEM((EXT, *wide), F32),
            pltpu.VMEM((4, EXT, *wide), F32), pltpu.VMEM((FIELDS, 3, *thin), F32),
            pltpu.VMEM((3, 2, *thin), F32), pltpu.VMEM((3, 3, *thin), F32),
            pltpu.VMEM((3, 2, *thin), F32), pltpu.VMEM((3, 3, *thin), F32),
            pltpu.VMEM((3, *thin), F32), pltpu.VMEM((3, *thin), F32), pltpu.VMEM((2, *thin), F32),
            pltpu.VMEM((FIELDS, 3, *thin), F32),
            pltpu.SemaphoreType.DMA((48,)), pltpu.SemaphoreType.DMA((21,)), pltpu.SemaphoreType.DMA((21,)),
            pltpu.SemaphoreType.REGULAR,
        ],
        compiler_params=pltpu.CompilerParams(collective_id=0, has_side_effects=True, vmem_limit_bytes=grant),
    )(*args)
    outs = [(2, LEVELS, ROWS, 2 * LANES), (LEVELS, ROWS, 2 * LANES), (LEVELS, ROWS, 2 * LANES), (3, LEVELS, ROWS, 2 * LANES)]
    return tuple(
        pl.pallas_call(
            output_kernel,
            out_shape=[jax.ShapeDtypeStruct(s, F32) for s in outs],
            in_specs=[whole] * len(passed),
            out_specs=[anywhere] * 4,
            scratch_shapes=[
                pltpu.VMEM((2, ROWS + 1, *wide), F32), pltpu.VMEM((ROWS, *wide), F32),
                pltpu.VMEM((ROWS, *wide), F32), pltpu.VMEM((3, ROWS, *wide), F32), pltpu.VMEM((ROWS, *thin), F32),
                pltpu.SemaphoreType.DMA((48,)),
            ],
            compiler_params=pltpu.CompilerParams(vmem_limit_bytes=grant),
        )(*between)
    )


def solution(mesh):
    edges, cell = P(None, None, "py", "px"), P(None, "py", "px")
    return jax.shard_map(
        local,
        mesh=mesh,
        in_specs=(edges, cell, edges, cell, cell, cell, P("py", "px"), edges, cell),
        out_specs=(edges, cell, cell, edges),
        check_vma=False,
    )
```

```python
import jax
import jax.numpy as jnp
from jax import lax
from jax.experimental import pallas as pl
from jax.experimental.pallas import tpu as pltpu
from jax.sharding import PartitionSpec as P

F32 = jnp.float32
MESH = pl.DeviceIdType.MESH
ROWS = 32
EXT = ROWS + 4
LEVELS = 8
LANES = 128

FIRST = (-2, 12, 26)
FIELDS = 10
GROUP = 6

DOWN, UP, RIGHT, LEFT = (1, 0), (-1, 0), (0, 1), (0, -1)
DOWN_LEFT, UP_LEFT, UP_RIGHT = (1, -1), (-1, -1), (-1, 1)


def rim_of(row):
    block = 0 if row <= 12 else (1 if row <= 26 else 2)
    return block, (row - FIRST[block]) * 8


def lane_id():
    return lax.broadcasted_iota(jnp.int32, (LEVELS, LANES), 1)


def turn(x, amount):
    amount = amount % LANES
    return x if amount == 0 else pltpu.roll(x, amount, 1)


def next_col(pair, lane):
    first, second = turn(pair[0], -1), turn(pair[1], -1)
    return jnp.where(lane == LANES - 1, second, first), second


def prev_col(pair, lane):
    first, second = turn(pair[0], 1), turn(pair[1], 1)
    return first, jnp.where(lane == 0, first, second)


def tile(t):
    return pl.ds(t * LANES, LANES)


def row_pair(ref, *index):
    return ref[(*index, slice(None), tile(0))], ref[(*index, slice(None), tile(1))]


def spread(ref, row, plane, t):
    return jnp.broadcast_to(ref[row, pl.ds(plane, 1), tile(t)], (LEVELS, LANES))


def spread_pair(ref, row, plane):
    return spread(ref, row, plane, 0), spread(ref, row, plane, 1)


def both(fn, *pairs):
    return tuple(fn(*(p[t] for p in pairs)) for t in range(2))


def add(a, b):
    return a + b


def mul(a, b):
    return a * b


def staged(rows, begin, finish, depth):
    waiting = []
    for row in rows:
        waiting.append((row, begin(row)))
        if len(waiting) > depth:
            finish(*waiting.pop(0))
    for row, value in waiting:
        finish(row, value)


def weigh(n0, n1, s0, s1):
    start = n0 / s0
    middle = (n0 + n0 + n1) / (s0 + s0 + s1)
    end = (n0 + n1) / (s0 + s1)
    twice = middle + middle
    late = twice + end
    return (start + twice + late) * (1.0 / 6.0), late * (1.0 / 6.0)


def first_vertex(cor, k0, k1, k2, f0, f1, f2_down, g0, g1, g2_down, h, h_down, h_right, m, m_down, m_right):
    n0 = cor * (k0 + k1 + k2) + (f0 + f2_down - f1)
    n1 = g0 + g2_down - g1
    s0 = k0 * h + k1 * h_down + k2 * h_right
    s1 = k0 * m + k1 * m_down + k2 * m_right
    return weigh(n0, n1, s0, s1)


def second_vertex(cor, k0, k1, k2, f1, f2, f0_diag, g1, g2, g0_diag, h, h_right, h_diag, m, m_right, m_diag):
    n0 = cor * (k0 + k1 + k2) + (f1 - f2 - f0_diag)
    n1 = g1 - g2 - g0_diag
    s0 = k0 * h + k1 * h_right + k2 * h_diag
    s1 = k0 * m + k1 * m_right + k2 * m_diag
    return weigh(n0, n1, s0, s1)


def energy_of(v, w, d, e):
    return (v * (v + w) + (w * w) * (1.0 / 3.0)) * (0.25 * d * e)


def turned_rows(rows, v, h, w, m, ga, right):
    def begin(row):
        d0 = spread_pair(ga, row, 0)
        pairs = (both(mul, row_pair(v, 0, row), d0), both(mul, row_pair(w, 0, row), d0), row_pair(h, row), row_pair(m, row))
        return [(turn(p[0], -1), turn(p[1], -1)) for p in pairs]

    def finish(row, turned):
        last = lane_id() == LANES - 1
        for n, (first, second) in enumerate(turned):
            right[n, row, :, tile(0)] = jnp.where(last, second, first)
            right[n, row, :, tile(1)] = second

    staged(rows, begin, finish, 8)


def vertex_rows(rows, v, h, w, m, ga, gb, right, out, depth=2, skip_first=None, skip_second=None):
    known = {}

    def flux(ref, name, k, row, key):
        if (name, k, key) not in known:
            known[name, k, key] = both(mul, row_pair(ref, k, row), spread_pair(ga, row, k))
        return known[name, k, key]

    def begin(item):
        key, row = item
        f = [flux(v, "v", k, row, key) for k in range(3)]
        g = [flux(w, "w", k, row, key) for k in range(3)]
        hh, mm = row_pair(h, row), row_pair(m, row)
        h_right, m_right = row_pair(right, 2, row), row_pair(right, 3, row)
        results = []
        if key != skip_first:
            below = row + 1
            f2_down, g2_down = flux(v, "v", 2, below, key + 1), flux(w, "w", 2, below, key + 1)
            h_down, m_down = row_pair(h, below), row_pair(m, below)
            cor = spread_pair(ga, row, 4)
            kite = [spread_pair(gb, row, p) for p in range(3)]
            for t in range(2):
                pair = first_vertex(
                    cor[t], kite[0][t], kite[1][t], kite[2][t], f[0][t], f[1][t], f2_down[t], g[0][t], g[1][t],
                    g2_down[t], hh[t], h_down[t], h_right[t], mm[t], m_down[t], m_right[t],
                )
                results += [(0, t, pair[0]), (1, t, pair[1])]
        if key != skip_second:
            above = row - 1
            f0_diag, g0_diag, h_diag, m_diag = (row_pair(right, n, above) for n in range(4))
            cor = spread_pair(ga, row, 5)
            kite = [spread_pair(gb, row, p) for p in range(3, 6)]
            for t in range(2):
                pair = second_vertex(
                    cor[t], kite[0][t], kite[1][t], kite[2][t], f[1][t], f[2][t], f0_diag[t], g[1][t], g[2][t],
                    g0_diag[t], hh[t], h_right[t], h_diag[t], mm[t], m_right[t], m_diag[t],
                )
                results += [(2, t, pair[0]), (3, t, pair[1])]
        return results

    def finish(item, results):
        for n, t, value in results:
            out[n, item[1], :, tile(t)] = value

    staged(rows, begin, finish, depth)


def cell_rows(rows, sums, out):
    def begin(row):
        values = []
        for n in range(2):
            v0, v1 = row_pair(sums, n, row), row_pair(sums, 2 + n, row)
            above, below = row_pair(sums, n, row - 1), row_pair(sums, 2 + n, row + 1)
            here = both(add, v0, v1)
            west = both(add, here, below)
            values.append((both(add, here, above), (turn(west[0], 1), turn(west[1], 1))))
        return values

    def finish(row, values):
        start = lane_id() == 0
        for n, (near, west) in enumerate(values):
            out[n, row, :, tile(0)] = (near[0] + west[0]) * (1.0 / 6.0)
            out[n, row, :, tile(1)] = (near[1] + jnp.where(start, west[0], west[1])) * (1.0 / 6.0)

    staged(rows, begin, finish, 5)


def side_rows(cell_at, vertex_at, cell, sums, right, corner):
    def begin(item):
        ref, row, back = item
        pair = row_pair(*ref, row)
        amount = 1 if back else -1
        return turn(pair[0], amount), turn(pair[1], amount)

    def finish(item, values):
        (_, n), row, back = item
        lane = lane_id()
        if back:
            corner[row - 3, :, tile(0)] = values[0]
            corner[row - 3, :, tile(1)] = jnp.where(lane == 0, values[0], values[1])
        else:
            right[n, row - 1, :, tile(0)] = jnp.where(lane == LANES - 1, values[1], values[0])
            right[n, row - 1, :, tile(1)] = values[1]

    items = [((sums, 2), row, True) for row in vertex_at]
    items += [((cell, n), row, False) for row in cell_at for n in range(2)]
    staged(items, begin, finish, 12)


def energy_rows(rows, v, w, ga, gb, inverse, out):
    spots = ((ga, 6), (ga, 7), (gb, 6))
    known = {}

    def one(k, row):
        if (k, row) not in known:
            ref, plane = spots[k]
            known[k, row] = both(
                energy_of, row_pair(v, k, row), row_pair(w, k, row), spread_pair(ga, row, k), spread_pair(ref, row, plane)
            )
        return known[k, row]

    def begin(row):
        e1 = one(1, row)
        near = both(lambda a, b, c, d: a + b + (c + d), one(0, row), one(0, row - 1), e1, one(2, row))
        west = both(add, e1, one(2, row + 1))
        return near, (turn(west[0], 1), turn(west[1], 1))

    def finish(row, values):
        near, west = values
        start = lane_id() == 0
        area = spread_pair(inverse, row, 3)
        out[row - 2, :, tile(0)] = (near[0] + west[0]) * area[0]
        out[row - 2, :, tile(1)] = (near[1] + jnp.where(start, west[0], west[1])) * area[1]

    staged(rows, begin, finish, 6)


def exchange_kernel(
    v_in, h_in, w_in, m_in, cd_in, el_in, ca_in, ka_in, co_in,
    v, w, sums, cell, kin, inverse, side, corner, rim_patch, rim_c, rim_right,
    h, m, ga, gb, turned, own, to_right, to_left, from_left, from_right, corner_tr, corner_br, corner_bl, rim,
    load_sem, send_sem, recv_sem, left_sem,
):
    ny, nx = lax.axis_size("py"), lax.axis_size("px")
    my, mx = lax.axis_index("py"), lax.axis_index("px")

    def device(dy, dx):
        return {"py": lax.rem(my + dy + ny, ny), "px": lax.rem(mx + dx + nx, nx)}

    barrier = pltpu.get_barrier_semaphore()

    def tell(sem, target):
        pl.semaphore_signal(sem, inc=1, device_id=device(*target), device_id_type=MESH)

    for target in (DOWN, UP, LEFT, DOWN_LEFT):
        tell(barrier, target)

    loads = []

    def load(src, dst):
        loads.append(pltpu.make_async_copy(src, dst, load_sem.at[len(loads)]))
        loads[-1].start()

    mine = pl.ds(2, ROWS)
    for p in range(3):
        load(cd_in.at[p], ga.at[mine, p])
    load(ca_in, ga.at[mine, 3])
    for p in range(2):
        load(co_in.at[p], ga.at[mine, 4 + p])
        load(el_in.at[p], ga.at[mine, 6 + p])
    for a in range(2):
        for p in range(3):
            load(ka_in.at[a, p], gb.at[mine, 3 * a + p])
    load(el_in.at[2], gb.at[mine, 6])
    load(el_in.at[2], gb.at[mine, 7])
    steps = [len(loads)]
    for src, dst in ((h_in, h), (m_in, m)):
        for k in range(LEVELS):
            load(src.at[k], dst.at[mine, k])
    steps.append(len(loads))
    for src, dst in ((v_in, v), (w_in, w)):
        for k in range(LEVELS):
            load(src.at[:, k], dst.at[:, mine, k])
        steps.append(len(loads))

    def arrived(step):
        for copy in loads[steps[step - 1] if step else 0 : steps[step]]:
            copy.wait()

    lane = lane_id()
    slot = lane & 7

    def field(f, row, t):
        if f < 3:
            return v[f, row, :, tile(t)]
        if f < 6:
            return w[f - 3, row, :, tile(t)]
        return (h, m, ga, gb)[f - 6][row, :, tile(t)]

    def strip(f, e):
        return jnp.where(lane >= 64, field(f, e, 1), field(f, e, 0))

    total = {}

    def gather(fields):
        for b in (2, 0, 1):
            rows = [r for r in range(FIRST[b], FIRST[b] + 16) if 0 <= r < ROWS]
            masks = [(lane >= (r - FIRST[b]) * 8) & (lane < (r - FIRST[b]) * 8 + 4) for r in rows]
            for f in fields:
                x = jnp.zeros((LEVELS, LANES), F32)
                for r, mask in zip(rows, masks):
                    x = jnp.where(mask, turn(strip(f, r + 2), (r - FIRST[b]) * 8 - 126), x)
                total[f, b] = x

    arrived(0)
    gather((8, 9))
    arrived(1)
    gather((6, 7))
    arrived(2)
    gather((0, 1, 2))
    arrived(3)

    pl.semaphore_wait(barrier, 4)
    tell(left_sem, RIGHT)

    sends = []

    def send(src, dst, target):
        n = len(sends)
        sends.append(
            pltpu.make_async_remote_copy(
                src_ref=src, dst_ref=dst, send_sem=send_sem.at[n], recv_sem=recv_sem.at[n],
                device_id=device(*target), device_id_type=MESH,
            )
        )
        sends[-1].start()
        return sends[-1]

    top, bottom = pl.ds(0, 2), pl.ds(EXT - 2, 2)
    last, lead = pl.ds(ROWS, 2), pl.ds(2, 2)
    row_sends, rim_sends = [], []
    for ref in (v, w):
        row_sends.append(send(ref.at[0:2, last], ref.at[0:2, top], DOWN))
        row_sends.append(send(ref.at[1:3, lead], ref.at[1:3, bottom], UP))
        row_sends.append(send(ref.at[2, ROWS + 1], ref.at[2, 1], DOWN))
        row_sends.append(send(ref.at[0, 2], ref.at[0, EXT - 2], UP))
    for ref in (h, m, ga, gb):
        row_sends.append(send(ref.at[last], ref.at[top], DOWN))
        row_sends.append(send(ref.at[lead], ref.at[bottom], UP))
    gather((3, 4, 5))
    packs = {}
    for b in (2, 0, 1):
        for s in range(3):
            x = jnp.zeros((LEVELS, LANES), F32)
            for f in range(4 * s, min(4 * s + 4, FIELDS)):
                at = 2 * (f - 4 * s)
                x = jnp.where((slot >> 1) == f - 4 * s, turn(total[f, b], at - 2), x)
            packs[1, b, s] = x
        for s in range(2):
            x = jnp.zeros((LEVELS, LANES), F32)
            for f in range(8 * s, min(8 * s + 8, FIELDS)):
                x = jnp.where(slot == f - 8 * s, turn(total[f, b], f - 8 * s - 1), x)
            packs[0, b, s] = x
    for (n, b, s), x in packs.items():
        (to_right, to_left)[n][b, s] = x
    for (f, b), x in total.items():
        own[f, b] = x

    def invert(row):
        return [1.0 / ga[row, :, tile(t)] for t in range(2)]

    def keep(row, values):
        for t in range(2):
            inverse[row, :, tile(t)] = values[t]

    staged(range(2, ROWS + 2), invert, keep, 8)
    rim_sends.append(send(to_right.at[0], corner_bl, UP_RIGHT))
    rim_sends.append(send(to_right, from_left, RIGHT))

    turned_rows(range(2, ROWS + 2), v, h, w, m, ga, turned)
    energy_rows(range(3, ROWS + 1), v, w, ga, gb, inverse, kin)
    pl.semaphore_wait(left_sem, 1)
    rim_sends.append(send(to_left.at[2], corner_tr, DOWN_LEFT))
    rim_sends.append(send(to_left, from_right, LEFT))
    rim_sends.append(send(to_left.at[0], corner_br, UP_LEFT))

    def group(index, _):
        base = 3 + index * GROUP
        vertex_rows([(j, base + j) for j in range(GROUP)], v, h, w, m, ga, gb, turned, sums)
        return 0

    lax.fori_loop(0, (ROWS - 2) // GROUP, group, 0)
    cell_rows(range(4, ROWS), sums, cell)
    side_rows(range(4, ROWS), range(3, ROWS + 1), cell, sums, side, corner)

    for copy in row_sends:
        copy.wait_recv()
    turned_rows((0, 1, EXT - 2, EXT - 1), v, h, w, m, ga, turned)
    vertex_rows([(e, e) for e in (0, 1, 2, ROWS + 1, ROWS + 2, ROWS + 3)], v, h, w, m, ga, gb, turned, sums, 2, EXT - 1, 0)
    energy_rows((2, ROWS + 1), v, w, ga, gb, inverse, kin)
    cell_rows((1, 2, 3, ROWS, ROWS + 1, ROWS + 2), sums, cell)
    side_rows((1, 2, 3, ROWS, ROWS + 1), (ROWS + 1, ROWS + 2), cell, sums, side, corner)
    merged = {}
    for b in range(3):
        for f in range(FIELDS):
            x = own[f, b]
            for r in ((-2, -1) if b == 0 else ((32, 33) if b == 2 else ())):
                q = (r - FIRST[b]) * 8
                x = jnp.where((lane >= q) & (lane < q + 4), turn(strip(f, r + 2), q - 126), x)
            merged[f, b] = jnp.where(slot < 2, x, turn(x, 3))
    for (f, b), x in merged.items():
        own[f, b] = x

    for copy in rim_sends:
        copy.wait_recv()

    top_rows, bottom_rows = lane < 16, (lane >= 48) & (lane < 64)
    strips = {}
    for b in range(3):
        right = [from_right[b, s] for s in range(3)]
        left = [from_left[b, s] for s in range(2)]
        if b == 0:
            right = [jnp.where(top_rows, turn(corner_tr[s], -32), right[s]) for s in range(3)]
        if b == 2:
            right = [jnp.where(bottom_rows, turn(corner_br[s], 32), right[s]) for s in range(3)]
            left = [jnp.where(bottom_rows, turn(corner_bl[s], 32), left[s]) for s in range(2)]
        for f in range(FIELDS):
            y = turn(right[f // 4], 2 - 2 * (f % 4))
            z = turn(left[f // 8], 4 - f % 8)
            strips[f, b] = jnp.where((slot >> 1) == 1, y, jnp.where(slot == 4, z, own[f, b]))
    for (f, b), x in strips.items():
        rim[f, b] = x

    results = {}

    def shift(x, di, dj):
        return turn(x, -(8 * di + dj))

    for b in range(3):

        def geo(f, plane):
            return jnp.broadcast_to(rim[f, b, pl.ds(plane, 1), :], (LEVELS, LANES))

        vv, ww = [rim[k, b] for k in range(3)], [rim[3 + k, b] for k in range(3)]
        hh, mm = rim[6, b], rim[7, b]
        d = [geo(8, k) for k in range(3)]
        f = [vv[k] * d[k] for k in range(3)]
        g = [ww[k] * d[k] for k in range(3)]
        h_right, m_right = shift(hh, 0, 1), shift(mm, 0, 1)
        v0, w0 = first_vertex(
            geo(8, 4), geo(9, 0), geo(9, 1), geo(9, 2), f[0], f[1], shift(f[2], 1, 0), g[0], g[1], shift(g[2], 1, 0),
            hh, shift(hh, 1, 0), h_right, mm, shift(mm, 1, 0), m_right,
        )
        v1, w1 = second_vertex(
            geo(8, 5), geo(9, 3), geo(9, 4), geo(9, 5), f[1], f[2], shift(f[0], -1, 1), g[1], g[2], shift(g[0], -1, 1),
            hh, h_right, shift(hh, -1, 1), mm, m_right, shift(mm, -1, 1),
        )
        length = (geo(8, 6), geo(8, 7), geo(9, 6))
        e = [energy_of(vv[k], ww[k], d[k], length[k]) for k in range(3)]
        energy = (e[0] + e[1] + e[2] + shift(e[0], -1, 0) + (shift(e[1], 0, -1) + shift(e[2], 1, -1))) / geo(8, 3)
        results[0, 0, b] = jnp.where(slot == 0, shift(v0, 0, 1), shift(energy, 0, 4))
        results[0, 1, b] = jnp.where(slot == 0, shift(v1, 0, 1), shift(v1, 1, 3))
        for n, (x0, x1) in enumerate(((v0, v1), (w0, w1))):
            here = x0 + x1
            mean = (here + shift(x0, -1, 0) + (shift(here, 0, -1) + shift(x1, 1, -1))) * (1.0 / 6.0)
            results[1, n, b] = jnp.where(slot == 0, shift(mean, 0, 1), shift(mean, 0, 4))
            results[2, n, b] = mean
    for (which, n, b), x in results.items():
        (rim_patch, rim_c, rim_right)[which][n, b] = x

    for copy in sends:
        copy.wait_send()


def output_kernel(
    v, w, sums, cell, kin, inverse, side, corner, rim_patch, rim_c, rim_right,
    vertex_out, kinetic_out, cell_out, edge_out,
    vertex_buf, kinetic_buf, cell_buf, edge_buf, corner_buf, sem,
):
    lane = lane_id()
    is_last, is_first, tail = lane == LANES - 1, lane == 0, lane >= LANES - 2

    def pick(ref, n, row, s, to):
        block, q = rim_of(row)
        return turn(ref[n, block], to - (q + s))

    copies = []

    def put(src, dst):
        copies.append(pltpu.make_async_copy(src, dst, sem.at[len(copies)]))
        copies[-1].start()

    def begin_patch(r):
        values = [row_pair(sums, 0, r + 2), pick(rim_patch, 0, r, 0, LANES - 1)]
        if r >= 0:
            values += [row_pair(sums, 2, r + 2), row_pair(kin, r), pick(rim_patch, 1, r, 0, LANES - 1)]
        return values

    def finish_patch(r, values):
        v0, patch = values[0:2]
        vertex_buf[0, r + 1, :, tile(0)] = v0[0]
        vertex_buf[0, r + 1, :, tile(1)] = jnp.where(is_last, patch, v0[1])
        if r >= 0:
            v1, energy, other = values[2:5]
            kinetic_buf[r, :, tile(0)] = jnp.where(is_first, patch, energy[0])
            kinetic_buf[r, :, tile(1)] = energy[1]
            vertex_buf[1, r + 1, :, tile(0)] = v1[0]
            vertex_buf[1, r + 1, :, tile(1)] = jnp.where(is_last, other, v1[1])
            corner_buf[r] = other

    staged(range(-1, ROWS), begin_patch, finish_patch, 8)
    for k in range(LEVELS):
        put(vertex_buf.at[:, 1 : ROWS + 1, k], vertex_out.at[:, k])
        put(kinetic_buf.at[:, k], kinetic_out.at[k])

    def begin(r):
        picks = [(pick(rim_c, n, r, 0, LANES - 1), pick(rim_right, n, r, 1, LANES - 2)) for n in range(2)]
        return picks

    cells, sides = {}, {}

    def work(r, picks):
        stores = []
        cells[r] = []
        sides[r] = []
        for n, (patch, patch_side) in enumerate(picks):
            pair = row_pair(cell, n, r + 2)
            cells[r].append((jnp.where(is_first, patch, pair[0]), jnp.where(is_last, patch, pair[1])))
            if r < ROWS:
                pair = row_pair(side, n, r + 1)
                sides[r].append((pair[0], jnp.where(tail, patch_side, pair[1])))
        if 0 <= r < ROWS:
            stores += [(cell_buf, (r,), t, cells[r][0][t]) for t in range(2)]
        q = r - 1
        if q >= 0:
            v0, v1, above = row_pair(vertex_buf, 0, q + 1), row_pair(vertex_buf, 1, q + 1), row_pair(vertex_buf, 0, q)
            back = row_pair(corner, q)
            means = (both(add, v0, (jnp.where(is_first, corner_buf[q], back[0]), back[1])), both(add, v0, v1), both(add, v1, above))
            here = cells[q]
            for k, other in enumerate((cells[r], sides[q], sides[q - 1])):
                velocity, tendency = row_pair(v, k, q + 2), row_pair(w, k, q + 2)
                factor = spread_pair(inverse, q + 2, k)
                for t in range(2):
                    slope = velocity[t] * (other[0][t] - here[0][t]) + tendency[t] * (other[1][t] - here[1][t])
                    stores.append((edge_buf, (k, q), t, 0.5 * (means[k][t] - slope * factor[t])))
        return stores

    def keep(stores):
        for ref, index, t, value in stores:
            ref[(*index, slice(None), tile(t))] = value

    half = ROWS // 2
    rows = list(range(-1, ROWS + 1))
    ahead = {r: begin(r) for r in rows[:8]}
    behind = []
    for r in rows:
        if r + 8 <= ROWS:
            ahead[r + 8] = begin(r + 8)
        behind.append(work(r, ahead.pop(r)))
        if len(behind) > 2:
            keep(behind.pop(0))
        if r in (half, ROWS):
            while behind:
                keep(behind.pop(0))
            part = pl.ds(r - half, half)
            for k in range(LEVELS):
                put(edge_buf.at[:, part, k], edge_out.at[:, k, part])
            for k in range(LEVELS):
                put(cell_buf.at[part, k], cell_out.at[k, part])
    for copy in copies:
        copy.wait()


def local(*args):
    args = [pltpu.with_memory_space_constraint(x, pltpu.HBM) for x in args]
    whole = pl.BlockSpec(memory_space=pltpu.VMEM)
    anywhere = pl.BlockSpec(memory_space=pl.ANY)
    wide = (LEVELS, 2 * LANES)
    thin = (LEVELS, LANES)
    passed = [
        (3, EXT, *wide), (3, EXT, *wide), (4, EXT, *wide), (2, EXT, *wide), (ROWS, *wide), (EXT, *wide),
        (2, ROWS + 1, *wide), (ROWS, *wide),
        (2, 3, *thin), (2, 3, *thin), (2, 3, *thin),
    ]
    grant = 24 << 20
    between = pl.pallas_call(
        exchange_kernel,
        out_shape=[pltpu.VMEM(s, F32) for s in passed],
        in_specs=[anywhere] * 9,
        out_specs=[whole] * len(passed),
        scratch_shapes=[
            pltpu.VMEM((EXT, *wide), F32), pltpu.VMEM((EXT, *wide), F32),
            pltpu.VMEM((EXT, *wide), F32), pltpu.VMEM((EXT, *wide), F32),
            pltpu.VMEM((4, EXT, *wide), F32), pltpu.VMEM((FIELDS, 3, *thin), F32),
            pltpu.VMEM((3, 2, *thin), F32), pltpu.VMEM((3, 3, *thin), F32),
            pltpu.VMEM((3, 2, *thin), F32), pltpu.VMEM((3, 3, *thin), F32),
            pltpu.VMEM((3, *thin), F32), pltpu.VMEM((3, *thin), F32), pltpu.VMEM((2, *thin), F32),
            pltpu.VMEM((FIELDS, 3, *thin), F32),
            pltpu.SemaphoreType.DMA((48,)), pltpu.SemaphoreType.DMA((21,)), pltpu.SemaphoreType.DMA((21,)),
            pltpu.SemaphoreType.REGULAR,
        ],
        compiler_params=pltpu.CompilerParams(collective_id=0, has_side_effects=True, vmem_limit_bytes=grant),
    )(*args)
    outs = [(2, LEVELS, ROWS, 2 * LANES), (LEVELS, ROWS, 2 * LANES), (LEVELS, ROWS, 2 * LANES), (3, LEVELS, ROWS, 2 * LANES)]
    return tuple(
        pl.pallas_call(
            output_kernel,
            out_shape=[jax.ShapeDtypeStruct(s, F32) for s in outs],
            in_specs=[whole] * len(passed),
            out_specs=[anywhere] * 4,
            scratch_shapes=[
                pltpu.VMEM((2, ROWS + 1, *wide), F32), pltpu.VMEM((ROWS, *wide), F32),
                pltpu.VMEM((ROWS, *wide), F32), pltpu.VMEM((3, ROWS, *wide), F32), pltpu.VMEM((ROWS, *thin), F32),
                pltpu.SemaphoreType.DMA((48,)),
            ],
            compiler_params=pltpu.CompilerParams(vmem_limit_bytes=grant),
        )(*between)
    )


def solution(mesh):
    edges, cell = P(None, None, "py", "px"), P(None, "py", "px")
    return jax.shard_map(
        local,
        mesh=mesh,
        in_specs=(edges, cell, edges, cell, cell, cell, P("py", "px"), edges, cell),
        out_specs=(edges, cell, cell, edges),
        check_vma=False,
    )
```
